128 devices in a mesh: gy: 2 (over core), gx: 64 (over z, y, x).
Axes of the slice: x: 4, y: 4, z: 4, core: 2. Of those that a mesh axis runs over, the one named last changes fastest.
Arguments:
- basis_vectors: float32 [36, 256, 128, 256], P(None, 'gx', 'gy'), may hold values from -30 to 30, as said below
- reaction: float32 [256, 128, 256], P('gx', 'gy'), may hold values from 0.5 to 3
Outputs:
- new_vectors: float32 [4, 256, 128, 256], P(None, 'gx', 'gy')
- hessenberg: float32 [40, 4], replicated
The draws below stay inside these ranges and needn't reach their ends.
Inputs may be any that keep to these rules, and one draw needn't show every extreme that they name: `basis_vectors`: under the inner product the basis vectors are nearly orthonormal.
All inputs are finite; a program needn't handle non-finite values.
Results may differ from the reference program's by a relative error of at most 0.0003.
Values sent between devices are 32-bit elements; how exact they have to be, the bound alone decides.
A program may use at most 128 MiB of HBM per device.

```python
import math
import jax
import jax.numpy as jnp
from jax import lax

KEEP = 36
STEPS = 4
BASIS = 40
NX = 256
NY = 128
NZ = 256


WIND_SPEEDS = (0.9, 0.6, 0.4)


TILT_SHARE = 0.01


MIXING_SHARE = 0.003


RAMP_FACTOR = 3.0


def stencil_drawn(values, x_ext, y_ext, z_ext, reaction):
    summed = -reaction * values
    for position, extended in enumerate((x_ext, y_ext, z_ext)):
        count = values.shape[position]
        higher = lax.slice_in_dim(extended, 3, count + 3, axis=position)
        lower_one = lax.slice_in_dim(extended, 1, count + 1, axis=position)
        lower_two = lax.slice_in_dim(extended, 0, count, axis=position)
        wind_speed = WIND_SPEEDS[position]
        summed = summed + higher + lower_one - 2.0 * values - wind_speed * (3.0 * values - 4.0 * lower_one + lower_two) * 0.5
    return summed


def apply_operator_drawn(values, reaction):
    padded = jnp.pad(values, ((2, 1), (2, 1), (2, 1)))
    return stencil_drawn(values, padded[:, 2:-1, 2:-1], padded[2:-1, :, 2:-1], padded[2:-1, 2:-1, :], reaction)


def reaction_field(key):
    key_field = jax.random.fold_in(key, 7)
    shape = (NX, NY, NZ)
    return jax.random.uniform(key_field, shape, jnp.float32, 0.5, 3.0)


def draw_reaction(key, part):
    return reaction_field(key)


def rough_fields(key, count, plane_scale):
    shape = (count, NX, NY, NZ)
    values = jax.random.normal(key, shape, jnp.float32)
    return values * plane_scale


def draw_basis_vectors(key, part):
    key_list = jax.random.split(jax.random.fold_in(key, 11), 4)
    plane_index = jnp.arange(NX, dtype=jnp.float32).reshape(NX, 1, 1)
    plane_scale = jnp.exp(math.log(RAMP_FACTOR) * plane_index / float(NX - 1))
    plane_scale = plane_scale / jnp.sqrt(jnp.mean(plane_scale * plane_scale))
    seed_fields = rough_fields(key_list[0], 2, plane_scale)
    start_field = seed_fields[0] / jnp.sqrt(jnp.mean(seed_fields[0] * seed_fields[0]))
    image_field = apply_operator_drawn(start_field, reaction_field(key))
    tilted = image_field + TILT_SHARE * jnp.sqrt(jnp.mean(image_field * image_field)) * seed_fields[1]
    tilted = tilted - jnp.sum(tilted * start_field) / jnp.sum(start_field * start_field) * start_field
    tilted = tilted / jnp.sqrt(jnp.mean(tilted * tilted))
    row_fields = jnp.concatenate([start_field[None], tilted[None], rough_fields(key_list[1], KEEP - 2, plane_scale)], axis=0)
    gram_matrix = jnp.einsum('axyz,bxyz->ab', row_fields, row_fields, precision=lax.Precision.HIGHEST) / float(NX * NY * NZ)
    inverse = jnp.linalg.inv(jnp.linalg.cholesky(gram_matrix))
    moved_order = jnp.concatenate([jnp.arange(1, KEEP, dtype=jnp.int32), jnp.zeros((1,), jnp.int32)])
    shuffle = jnp.eye(KEEP, dtype=jnp.float32)[moved_order]
    mixing = jnp.eye(KEEP, dtype=jnp.float32) + MIXING_SHARE * jax.random.normal(key_list[2], (KEEP, KEEP), jnp.float32)
    matrix = jnp.dot(mixing, jnp.dot(shuffle, inverse, precision=lax.Precision.HIGHEST), precision=lax.Precision.HIGHEST)
    return jnp.einsum('ab,bxyz->axyz', matrix, row_fields, precision=lax.Precision.HIGHEST)


def setup_inputs(seed: int = 0) -> dict:
    splits = jax.random.split(jax.random.key(seed), 3)
    basis_vectors = draw_basis_vectors(jax.random.fold_in(splits[2], 71), 0)
    reaction = draw_reaction(jax.random.fold_in(splits[2], 71), 0)
    return {"basis_vectors": basis_vectors, "reaction": reaction}


WIND_SPEEDS = (0.9, 0.6, 0.4)
EPSILON = 1e-06

def stencil(values, x_ext, y_ext, z_ext, reaction):
    summed = -reaction * values
    for position, extended in enumerate((x_ext, y_ext, z_ext)):
        count = values.shape[position]
        higher = lax.slice_in_dim(extended, 3, count + 3, axis=position)
        lower_one = lax.slice_in_dim(extended, 1, count + 1, axis=position)
        lower_two = lax.slice_in_dim(extended, 0, count, axis=position)
        wind_speed = WIND_SPEEDS[position]
        summed = summed + higher + lower_one - 2.0 * values - wind_speed * (3.0 * values - 4.0 * lower_one + lower_two) * 0.5
    return summed

def apply_operator(values, reaction):
    padded = jnp.pad(values, ((2, 1), (2, 1), (2, 1)))
    return stencil(values, padded[:, 2:-1, 2:-1], padded[2:-1, :, 2:-1], padded[2:-1, 2:-1, :], reaction)

def project(basis_vectors, created, image):
    local = jnp.einsum('kxyz,xyz->k', basis_vectors, image, precision=lax.Precision.HIGHEST)
    extra = [jnp.sum(vector * image)[None] for vector in created]
    return jnp.concatenate([local] + extra)

def combine(basis_vectors, created, weights):
    keep_count = basis_vectors.shape[0]
    summed = jnp.einsum('k,kxyz->xyz', weights[:keep_count], basis_vectors, precision=lax.Precision.HIGHEST)
    for index, vector in enumerate(created):
        summed = summed + weights[keep_count + index] * vector
    return summed

def reference(basis_vectors, reaction):
    cell_count = float(NX * NY * NZ)
    created = []
    columns = []
    for section in range(STEPS):
        current = KEEP + section
        vector_now = basis_vectors[KEEP - 1] if section == 0 else created[-1]
        image = apply_operator(vector_now, reaction)
        first_terms = project(basis_vectors, created, image) / cell_count
        first_rest = image - combine(basis_vectors, created, first_terms)
        second_terms = project(basis_vectors, created, first_rest) / cell_count
        second_rest = first_rest - combine(basis_vectors, created, second_terms)
        length_now = jnp.sqrt(jnp.sum(second_rest * second_rest) / cell_count + EPSILON)
        columns.append(jnp.concatenate([first_terms + second_terms, length_now[None], jnp.zeros((BASIS - current - 1,), jnp.float32)]))
        created.append(second_rest / length_now)
    return (jnp.stack(created), jnp.stack(columns, axis=1))
```

```python
import functools

import jax
import jax.numpy as jnp
from jax import lax
from jax.experimental import pallas as pl
from jax.experimental.pallas import tpu as pltpu
from jax.sharding import PartitionSpec as P

MESH = pl.DeviceIdType.MESH
STEPS = 4
WIND = (0.9, 0.6, 0.4)
EPSILON = 1e-06
SIDE = 4
CHIPS = 64
DEVICES = 128
ROWS = 40


def hops(delta):
    return sum(min(d, SIDE - d) for d in delta[:3])


def partners(with_core):
    places = [
        (z, y, x, c)
        for z in range(SIDE)
        for y in range(SIDE)
        for x in range(SIDE)
        for c in range(2 if with_core else 1)
    ]
    return sorted(
        [p for p in places if any(p)], key=lambda p: (-hops(p), p[2], p[1], p[0])
    )


def kernel(
    keep,
    planes,
    rows,
    cols,
    basis,
    react,
    out,
    hess,
    V,
    W,
    RC,
    low_x,
    high_x,
    side_y,
    acc,
    acc_kept,
    gram_hh,
    gram_hl,
    gram_ll,
    hb,
    row_src,
    row_all,
    pair_src,
    pair_got,
    half_src,
    half_all,
    half_got,
    load_sem,
    x_send,
    low_recv,
    high_recv,
    y_send,
    y_recv,
    row_send,
    row_recv,
    gram_send,
    gram_recv,
):
    f32 = jnp.float32
    core = lax.axis_index("gy")
    chip = lax.axis_index("gx")
    me = core * CHIPS + chip
    cz, cy, cx = lax.div(chip, 16), lax.rem(lax.div(chip, 4), 4), lax.rem(chip, 4)
    zs = [lax.rem(cz + d, SIDE) * 16 for d in range(SIDE)]
    ys = [lax.rem(cy + d, SIDE) * 4 for d in range(SIDE)]
    xs = [lax.rem(cx + d, SIDE) for d in range(SIDE)]
    cores = [core, 1 - core]
    inv_cells = 1.0 / float(DEVICES * planes * rows * cols)

    def device(place):
        z, y, x, c = place
        return {"gy": cores[c], "gx": zs[z] + ys[y] + xs[x]}

    barrier = pltpu.get_barrier_semaphore()
    for place in partners(True):
        pl.semaphore_signal(
            barrier, inc=1, device_id=device(place), device_id_type=MESH
        )

    last = keep - 1
    loads = [
        pltpu.make_async_copy(basis.at[last], V.at[last], load_sem.at[0]),
        pltpu.make_async_copy(react, RC, load_sem.at[1]),
    ]
    for n, start in enumerate(range(0, last, 7)):
        part = pl.ds(start, min(7, last - start))
        loads.append(
            pltpu.make_async_copy(basis.at[part], V.at[part], load_sem.at[2 + n])
        )
    for copy in loads:
        copy.start()

    acc[...] = jnp.zeros(acc.shape, f32)
    acc_kept[...] = jnp.zeros(acc_kept.shape, f32)
    gram_hh[...] = jnp.zeros(gram_hh.shape, f32)
    gram_hl[...] = jnp.zeros(gram_hl.shape, f32)
    gram_ll[...] = jnp.zeros(gram_ll.shape, f32)

    @pl.when(chip == 0)
    def _():
        low_x[...] = jnp.zeros(low_x.shape, f32)

    @pl.when(chip == CHIPS - 1)
    def _():
        high_x[...] = jnp.zeros(high_x.shape, f32)

    loads[0].wait()
    pl.semaphore_wait(barrier, DEVICES - 1)

    def to_next(step, plane):
        return pltpu.make_async_remote_copy(
            V.at[last + step, plane],
            low_x.at[step, plane - (planes - 2)],
            x_send.at[step, plane - (planes - 2)],
            low_recv.at[step, plane - (planes - 2)],
            device_id={"gy": core, "gx": lax.rem(chip + 1, CHIPS)},
            device_id_type=MESH,
        )

    def to_previous(step):
        return pltpu.make_async_remote_copy(
            V.at[last + step, 0],
            high_x.at[step],
            x_send.at[step, 2],
            high_recv.at[step],
            device_id={"gy": core, "gx": lax.rem(chip + CHIPS - 1, CHIPS)},
            device_id_type=MESH,
        )

    edge = pl.ds(pl.multiple_of((1 - core) * (rows - 8), 8), 8)

    def to_side(step, plane):
        return pltpu.make_async_remote_copy(
            V.at[last + step, plane, edge],
            side_y.at[step, plane],
            y_send.at[step, plane],
            y_recv.at[step, plane],
            device_id={"gy": 1 - core, "gx": chip},
            device_id_type=MESH,
        )

    def send_plane(step, plane):
        if plane >= planes - 2:

            @pl.when(chip < CHIPS - 1)
            def _():
                to_next(step, plane).start()

        if plane == 0:

            @pl.when(chip > 0)
            def _():
                to_previous(step).start()

        to_side(step, plane).start()

    order = (3, 2, 0, 1)
    for plane in order:
        send_plane(0, plane)

    lanes = lax.broadcasted_iota(jnp.int32, (rows, cols), 1)

    def local_part(step):
        centre = 6.0 + 1.5 * sum(WIND)
        index = last + step
        for plane in range(planes):
            to_side(step, plane).wait_recv()
        for plane in range(planes):
            v = V[index, plane]
            side = side_y[step, plane]
            below = jnp.where(core == 1, side, 0.0)
            above = jnp.where(core == 0, side, 0.0)
            tall = jnp.concatenate([below, v, above], axis=0)
            total = -(RC[plane] + centre) * v
            s = WIND[1]
            total += tall[9 : rows + 9]
            total += (1.0 + 2.0 * s) * tall[7 : rows + 7] - (0.5 * s) * tall[6 : rows + 6]
            s = WIND[2]
            total += jnp.where(lanes < cols - 1, pltpu.roll(v, cols - 1, 1), 0.0)
            total += (1.0 + 2.0 * s) * jnp.where(lanes >= 1, pltpu.roll(v, 1, 1), 0.0)
            total -= (0.5 * s) * jnp.where(lanes >= 2, pltpu.roll(v, 2, 1), 0.0)
            s = WIND[0]
            if plane + 1 < planes:
                total += V[index, plane + 1]
            if plane >= 1:
                total += (1.0 + 2.0 * s) * V[index, plane - 1]
            if plane >= 2:
                total -= (0.5 * s) * V[index, plane - 2]
            W[plane] = total

    def far_part(step):
        s = WIND[0]

        @pl.when(chip > 0)
        def _():
            to_next(step, planes - 2).wait_recv()
            to_next(step, planes - 1).wait_recv()

        @pl.when(chip < CHIPS - 1)
        def _():
            to_previous(step).wait_recv()

        W[0] += (1.0 + 2.0 * s) * low_x[step, 1] - (0.5 * s) * low_x[step, 0]
        W[1] -= (0.5 * s) * low_x[step, 1]
        W[planes - 1] += high_x[step]

    def folded(product):
        half = product[:, : cols // 2] + product[:, cols // 2 :]
        parts = [half[8 * t : 8 * t + 8] for t in range(rows // 8)]
        while len(parts) > 1:
            parts = [a + b for a, b in zip(parts[::2], parts[1::2])]
        return parts[0]

    def project(operands, plane, count, target):
        def one(i):
            v = V[i, plane]
            for offset, w in operands:
                part = folded(v * w)
                target[offset + i] = part if plane == 0 else target[offset + i] + part

        whole = count // 4

        def four(t, carry):
            for q in range(4):
                one(4 * t + q)
            return carry

        lax.fori_loop(0, whole, four, 0)
        for i in range(4 * whole, count):
            one(i)

    def diagonal(shape):
        return lax.broadcasted_iota(jnp.int32, shape, 0) == lax.broadcasted_iota(
            jnp.int32, shape, 1
        )

    def as_row(column, count):
        return jnp.sum(
            jnp.where(diagonal((count, 128)), column, 0.0), axis=0, keepdims=True
        )

    def as_column(row):
        return jnp.sum(
            jnp.where(diagonal((ROWS, 128)), row, 0.0), axis=1, keepdims=True
        )

    def packed(ref, start, count):
        flat = jnp.sum(ref[start : start + count], axis=1)
        return as_row(jnp.sum(flat, axis=1, keepdims=True), count)

    def send_row(n, row):
        row_src[n] = row
        row_all[n, me] = row
        for place in partners(True):
            pltpu.make_async_remote_copy(
                row_src.at[n],
                row_all.at[n, me],
                row_send.at[n],
                row_recv.at[n],
                device_id=device(place),
                device_id_type=MESH,
            ).start()

    def row_bytes(n, sem):
        part = row_all.at[n, pl.ds(0, DEVICES - 1)]
        return pltpu.make_async_copy(part, part, sem.at[n])

    def get_row(n):
        row_bytes(n, row_recv).wait()
        return jnp.sum(row_all[n], axis=0) * inv_cells

    row_id = lax.broadcasted_iota(jnp.int32, (ROWS, 128), 0)
    lane_id = lax.broadcasted_iota(jnp.int32, (ROWS, 128), 1)
    lane_row = lax.broadcasted_iota(jnp.int32, (1, 128), 1)
    row_column = lax.broadcasted_iota(jnp.int32, (ROWS, 1), 0)

    loads[1].wait()
    local_part(0)
    for copy in loads[2:]:
        copy.wait()

    block = 32

    def gram_tile(t, carry):
        plane, tile = lax.div(t, rows // 8), lax.rem(t, rows // 8)
        start = pl.multiple_of(tile * 8, 8)
        v = V[0:block, plane, pl.ds(start, 8), :].reshape(block * 8, cols)
        high = v.astype(jnp.bfloat16)
        rest = v - high.astype(f32)
        low = rest.astype(jnp.bfloat16)
        contract = (((1,), (1,)), ((), ()))
        gram_hh[...] += lax.dot_general(
            high, high, contract, preferred_element_type=f32
        )
        gram_hl[...] += lax.dot_general(high, low, contract, preferred_element_type=f32)
        square = rest * rest
        gram_ll[...] += square[:, : cols // 2] + square[:, cols // 2 :]
        return carry

    lax.fori_loop(0, planes * (rows // 8), gram_tile, 0)
    for plane in range(planes):
        project([(0, V[32, plane]), (ROWS, V[33, plane])], plane, keep, acc_kept)
        project([(2 * ROWS, V[34, plane])], plane, keep, acc_kept)
    for plane in range(planes):
        project([(ROWS, V[last, plane])], plane, keep, acc)

    same = lax.rem(
        lax.broadcasted_iota(jnp.int32, (block * 8, block * 8), 0), 8
    ) == lax.rem(lax.broadcasted_iota(jnp.int32, (block * 8, block * 8), 1), 8)
    pick = (
        lax.div(lax.broadcasted_iota(jnp.int32, (block * 8, 128), 0), 8)
        == lax.broadcasted_iota(jnp.int32, (block * 8, 128), 1)
    ).astype(f32)

    def blocks(ref):
        kept = jnp.where(same, ref[...], 0.0).reshape(block, 8, block * 8)
        return jnp.dot(
            jnp.sum(kept, axis=1),
            pick,
            precision=lax.Precision.HIGHEST,
            preferred_element_type=f32,
        )

    hh, hl = blocks(gram_hh), blocks(gram_hl)
    ll = jnp.sum(
        jnp.sum(gram_ll[...].reshape(block, 8, 128), axis=1), axis=1, keepdims=True
    )
    hh = hh + jnp.where(diagonal((block, 128)), ll, 0.0)

    def dense(matrix):
        total = matrix[0:8]
        for q in range(1, 4):
            total = total + pltpu.roll(matrix[8 * q : 8 * q + 8], block * q, 1)
        return total

    pair_src[0:8] = dense(hh)
    pair_src[8:16] = dense(hl)
    for q in range(3):
        pair_src[16 + q : 17 + q] = packed(acc_kept, ROWS * q, ROWS)
    pair_src[19:32] = jnp.zeros((13, 128), f32)
    to_pair = pltpu.make_async_remote_copy(
        pair_src,
        pair_got,
        gram_send.at[0],
        gram_recv.at[0],
        device_id={"gy": 1 - core, "gx": chip},
        device_id_type=MESH,
    )
    to_pair.start()

    def finish_operator(step, count):
        far_part(step)
        for plane in range(planes):
            project([(0, W[plane])], plane, count, acc)
        send_row(step, packed(acc, 0, 2 * ROWS))

    finish_operator(0, keep)

    to_pair.wait_recv()
    chip_sum = pair_src[...] + pair_got[...]
    half = 16
    mine = jnp.where(core == 0, chip_sum[0:half], chip_sum[half : 2 * half])
    half_src[...] = mine
    half_all[chip] = mine
    for place in partners(False):
        pltpu.make_async_remote_copy(
            half_src,
            half_all.at[chip],
            gram_send.at[1],
            gram_recv.at[1],
            device_id=device(place),
            device_id_type=MESH,
        ).start()

    def half_bytes(sem):
        part = half_all.at[pl.ds(0, CHIPS - 1)]
        return pltpu.make_async_copy(part, part, sem.at[1])

    half_bytes(gram_recv).wait()
    mine = jnp.sum(half_all[...], axis=0) * inv_cells
    pair_src2 = half_got.at[0]
    pair_src2[...] = mine
    swap = pltpu.make_async_remote_copy(
        half_got.at[0],
        half_got.at[1],
        gram_send.at[2],
        gram_recv.at[2],
        device_id={"gy": 1 - core, "gx": chip},
        device_id_type=MESH,
    )
    swap.start()
    swap.wait_recv()
    first_half = jnp.where(core == 0, half_got[0], half_got[1])
    second_half = jnp.where(core == 0, half_got[1], half_got[0])

    def spread(packed_block):
        parts = [packed_block] + [
            pltpu.roll(packed_block, 128 - block * q, 1) for q in range(1, 4)
        ]
        full = jnp.concatenate(parts, axis=0)
        return jnp.where(
            lax.broadcasted_iota(jnp.int32, (block, 128), 1) < block, full, 0.0
        )

    hh, hl = spread(first_half[0:8]), spread(first_half[8:16])
    turned = jnp.concatenate([hl, jnp.zeros((96, 128), f32)], axis=0).T[0:block]
    gram = jnp.concatenate([hh + hl + turned, jnp.zeros((8, 128), f32)], axis=0)
    for q in range(3):
        values = second_half[q : q + 1]
        gram = jnp.where(row_id == block + q, values, gram)
    for q in range(3):
        values = as_column(second_half[q : q + 1])
        gram = jnp.where(lane_id == block + q, values, gram)
    eye = jnp.where(row_id == lane_id, 2.0, 0.0)
    lower = jnp.logical_and(row_id < last, lane_id < last)
    matrix = jnp.where(lower, eye - gram, 0.0)

    scale_row = jnp.ones((1, 128), f32)
    scale_column = jnp.ones((ROWS, 1), f32)
    results = jnp.zeros((ROWS, 128), f32)
    inverse = None
    for step in range(STEPS):
        count = keep + step
        if step > 0:
            local_part(step)
            for plane in range(planes):
                project([(ROWS, V[last + step, plane])], plane, count, acc)
            if step > 1:
                for plane in range(planes):
                    out[step - 2, plane] = V[last + step - 1, plane] * inverse
            finish_operator(step, count)
        sums = get_row(step)
        if step > 0:
            square = jnp.sum(
                jnp.where(lane_row == ROWS + count - 1, sums, 0.0),
                axis=1,
                keepdims=True,
            )
            norm = jnp.sqrt(square + EPSILON)
            inverse = 1.0 / norm
            scale_row = jnp.where(lane_row == count - 1, inverse, scale_row)
            scale_column = jnp.where(row_column == count - 1, inverse, scale_column)
            results = jnp.where(
                jnp.logical_and(row_id == count - 1, lane_id == step - 1), norm, results
            )
            factor = scale_row * inverse
        else:
            factor = scale_row
        valid = lane_row < count
        first = jnp.where(valid, sums * factor, 0.0)
        cross = jnp.where(valid, pltpu.roll(sums, 128 - ROWS, 1) * factor, 0.0)
        cross_column = as_column(cross)
        matrix = jnp.where(row_id == count - 1, eye - cross, matrix)
        matrix = jnp.where(lane_id == count - 1, eye - cross_column, matrix)
        weights = jnp.sum(matrix * first, axis=1, keepdims=True)
        weights = jnp.where(row_column < count, weights, 0.0)
        results = jnp.where(lane_id == step, weights, results)
        hb[...] = jnp.broadcast_to(weights * scale_column, hb.shape)

        for plane in order:
            start = W[plane] if step == 0 else W[plane] * inverse

            def minus(i, total):
                return total - hb[pl.ds(i, 1), :] * V[i, plane]

            def four(t, total):
                for q in range(4):
                    total = minus(4 * t + q, total)
                return total

            total = lax.fori_loop(0, count // 4, four, start)
            for i in range(4 * (count // 4), count):
                total = minus(i, total)
            V[count, plane] = total
            if step + 1 < STEPS:
                send_plane(step + 1, plane)

    total = jnp.zeros((8, 128), f32)
    for plane in range(planes):
        v = V[keep + STEPS - 1, plane]
        total = total + folded(v * v)
    square = jnp.sum(jnp.sum(total, axis=0, keepdims=True), axis=1, keepdims=True)
    send_row(STEPS, jnp.broadcast_to(square, (1, 128)))
    for plane in range(planes):
        out[STEPS - 2, plane] = V[keep + STEPS - 2, plane] * inverse
    sums = get_row(STEPS)
    norm = jnp.sqrt(sums[:, 0:1] + EPSILON)
    inverse = 1.0 / norm
    results = jnp.where(
        jnp.logical_and(row_id == keep + STEPS - 1, lane_id == STEPS - 1), norm, results
    )
    hess[...] = results[:, 0:STEPS]
    for plane in range(planes):
        out[STEPS - 1, plane] = V[keep + STEPS - 1, plane] * inverse

    for step in range(STEPS):

        @pl.when(chip < CHIPS - 1)
        def _():
            to_next(step, planes - 2).wait_send()
            to_next(step, planes - 1).wait_send()

        @pl.when(chip > 0)
        def _():
            to_previous(step).wait_send()

        for plane in range(planes):
            to_side(step, plane).wait_send()
    for n in range(STEPS + 1):
        row_bytes(n, row_send).wait()
    to_pair.wait_send()
    half_bytes(gram_send).wait()
    swap.wait_send()


def body(basis_vectors, reaction):
    keep, planes, rows, cols = basis_vectors.shape
    f32 = jnp.float32
    field = (planes, rows, cols)
    dma = pltpu.SemaphoreType.DMA
    vmem = pltpu.VMEM
    return pl.pallas_call(
        functools.partial(kernel, keep, planes, rows, cols),
        out_shape=(
            jax.ShapeDtypeStruct((STEPS, *field), f32),
            jax.ShapeDtypeStruct((keep + STEPS, STEPS), f32),
        ),
        in_specs=[pl.BlockSpec(memory_space=pl.ANY)] * 2,
        out_specs=(
            pl.BlockSpec(memory_space=pltpu.VMEM),
            pl.BlockSpec(memory_space=pltpu.VMEM),
        ),
        scratch_shapes=[
            vmem((keep + STEPS, *field), f32),
            vmem(field, f32),
            vmem(field, f32),
            vmem((STEPS, 2, rows, cols), f32),
            vmem((STEPS, rows, cols), f32),
            vmem((STEPS, planes, 8, cols), f32),
            vmem((2 * ROWS, 8, 128), f32),
            vmem((3 * ROWS, 8, 128), f32),
            vmem((256, 256), f32),
            vmem((256, 256), f32),
            vmem((256, 128), f32),
            vmem((ROWS, cols), f32),
            vmem((STEPS + 1, 1, 128), f32),
            vmem((STEPS + 1, DEVICES, 1, 128), f32),
            vmem((32, 128), f32),
            vmem((32, 128), f32),
            vmem((16, 128), f32),
            vmem((CHIPS, 16, 128), f32),
            vmem((2, 16, 128), f32),
            dma((9,)),
            dma((STEPS, 3)),
            dma((STEPS, 2)),
            dma((STEPS,)),
            dma((STEPS, planes)),
            dma((STEPS, planes)),
            dma((STEPS + 1,)),
            dma((STEPS + 1,)),
            dma((3,)),
            dma((3,)),
        ],
        compiler_params=pltpu.CompilerParams(
            collective_id=0,
            has_side_effects=True,
            vmem_limit_bytes=48 * 1024 * 1024,
        ),
    )(basis_vectors, reaction)


def solution(mesh):
    return jax.shard_map(
        body,
        mesh=mesh,
        in_specs=(P(None, "gx", "gy", None), P("gx", "gy", None)),
        out_specs=(P(None, "gx", "gy", None), P()),
        check_vma=False,
    )
```

```python
import functools

import jax
import jax.numpy as jnp
from jax import lax
from jax.experimental import pallas as pl
from jax.experimental.pallas import tpu as pltpu
from jax.sharding import PartitionSpec as P

MESH = pl.DeviceIdType.MESH
STEPS = 4
WIND = (0.9, 0.6, 0.4)
EPSILON = 1e-06
SIDE = 4
CHIPS = 64
DEVICES = 128
ROWS = 40


def hops(delta):
    return sum(min(d, SIDE - d) for d in delta[:3])


def partners(with_core):
    places = [
        (z, y, x, c)
        for z in range(SIDE)
        for y in range(SIDE)
        for x in range(SIDE)
        for c in range(2 if with_core else 1)
    ]
    return sorted(
        [p for p in places if any(p)], key=lambda p: (-hops(p), p[2], p[1], p[0])
    )


def kernel(
    keep,
    planes,
    rows,
    cols,
    basis,
    react,
    out,
    hess,
    V,
    W,
    RC,
    low_x,
    high_x,
    side_y,
    acc,
    acc_kept,
    gram_hh,
    gram_hl,
    gram_lh,
    gram_ll,
    hb,
    row_src,
    row_all,
    pair_src,
    pair_got,
    half_src,
    half_all,
    swap_buf,
    load_sem,
    x_send,
    low_recv,
    high_recv,
    y_send,
    y_recv,
    row_send,
    row_recv,
    gram_send,
    gram_recv,
):
    f32 = jnp.float32
    core = lax.axis_index("gy")
    chip = lax.axis_index("gx")
    me = core * CHIPS + chip
    cz, cy, cx = lax.div(chip, 16), lax.rem(lax.div(chip, 4), 4), lax.rem(chip, 4)
    zs = [lax.rem(cz + d, SIDE) * 16 for d in range(SIDE)]
    ys = [lax.rem(cy + d, SIDE) * 4 for d in range(SIDE)]
    xs = [lax.rem(cx + d, SIDE) for d in range(SIDE)]
    cores = [core, 1 - core]
    inv_cells = 1.0 / float(DEVICES * planes * rows * cols)

    def device(place):
        z, y, x, c = place
        return {"gy": cores[c], "gx": zs[z] + ys[y] + xs[x]}

    last = keep - 1
    loads = [
        pltpu.make_async_copy(basis.at[last], V.at[last], load_sem.at[0]),
        pltpu.make_async_copy(react, RC, load_sem.at[1]),
    ]
    for n, start in enumerate(range(0, last, 7)):
        part = pl.ds(start, min(7, last - start))
        loads.append(
            pltpu.make_async_copy(basis.at[part], V.at[part], load_sem.at[2 + n])
        )
    for copy in loads:
        copy.start()

    barrier = pltpu.get_barrier_semaphore()
    for place in partners(True):
        pl.semaphore_signal(
            barrier, inc=1, device_id=device(place), device_id_type=MESH
        )

    acc[...] = jnp.zeros(acc.shape, f32)
    acc_kept[...] = jnp.zeros(acc_kept.shape, f32)
    gram_hh[...] = jnp.zeros(gram_hh.shape, f32)
    gram_hl[...] = jnp.zeros(gram_hl.shape, f32)
    gram_lh[...] = jnp.zeros(gram_lh.shape, f32)
    gram_ll[...] = jnp.zeros(gram_ll.shape, f32)

    @pl.when(chip == 0)
    def _():
        low_x[...] = jnp.zeros(low_x.shape, f32)

    @pl.when(chip == CHIPS - 1)
    def _():
        high_x[...] = jnp.zeros(high_x.shape, f32)

    def to_next(step, plane):
        return pltpu.make_async_remote_copy(
            V.at[last + step, plane],
            low_x.at[step, plane - (planes - 2)],
            x_send.at[step, plane - (planes - 2)],
            low_recv.at[step, plane - (planes - 2)],
            device_id={"gy": core, "gx": lax.rem(chip + 1, CHIPS)},
            device_id_type=MESH,
        )

    def to_previous(step):
        return pltpu.make_async_remote_copy(
            V.at[last + step, 0],
            high_x.at[step],
            x_send.at[step, 2],
            high_recv.at[step],
            device_id={"gy": core, "gx": lax.rem(chip + CHIPS - 1, CHIPS)},
            device_id_type=MESH,
        )

    edge = pl.ds(pl.multiple_of((1 - core) * (rows - 8), 8), 8)

    def to_side(step, plane):
        return pltpu.make_async_remote_copy(
            V.at[last + step, plane, edge],
            side_y.at[step, plane],
            y_send.at[step, plane],
            y_recv.at[step, plane],
            device_id={"gy": 1 - core, "gx": chip},
            device_id_type=MESH,
        )

    def send_plane(step, plane):
        if plane >= planes - 2:

            @pl.when(chip < CHIPS - 1)
            def _():
                to_next(step, plane).start()

        if plane == 0:

            @pl.when(chip > 0)
            def _():
                to_previous(step).start()

        to_side(step, plane).start()

    order = (3, 2, 0, 1)

    lanes = lax.broadcasted_iota(jnp.int32, (rows, cols), 1)

    def local_part(step):
        centre = 6.0 + 1.5 * sum(WIND)
        index = last + step
        for plane in range(planes):
            to_side(step, plane).wait_recv()
        for plane in range(planes):
            v = V[index, plane]
            side = side_y[step, plane]
            below = jnp.where(core == 1, side, 0.0)
            above = jnp.where(core == 0, side, 0.0)
            tall = jnp.concatenate([below, v, above], axis=0)
            total = -(RC[plane] + centre) * v
            s = WIND[1]
            total += tall[9 : rows + 9]
            total += (1.0 + 2.0 * s) * tall[7 : rows + 7] - (0.5 * s) * tall[6 : rows + 6]
            s = WIND[2]
            total += jnp.where(lanes < cols - 1, pltpu.roll(v, cols - 1, 1), 0.0)
            total += (1.0 + 2.0 * s) * jnp.where(lanes >= 1, pltpu.roll(v, 1, 1), 0.0)
            total -= (0.5 * s) * jnp.where(lanes >= 2, pltpu.roll(v, 2, 1), 0.0)
            s = WIND[0]
            if plane + 1 < planes:
                total += V[index, plane + 1]
            if plane >= 1:
                total += (1.0 + 2.0 * s) * V[index, plane - 1]
            if plane >= 2:
                total -= (0.5 * s) * V[index, plane - 2]
            W[plane] = total

    def low_plane(step, plane):
        @pl.when(chip > 0)
        def _():
            to_next(step, plane).wait_recv()

    def high_plane(step):
        @pl.when(chip < CHIPS - 1)
        def _():
            to_previous(step).wait_recv()

    def folded(product):
        half = product[:, : cols // 2] + product[:, cols // 2 :]
        parts = [half[8 * t : 8 * t + 8] for t in range(rows // 8)]
        while len(parts) > 1:
            parts = [a + b for a, b in zip(parts[::2], parts[1::2])]
        return parts[0]

    def project(operands, plane, target, first, count, fresh):
        def one(i):
            v = V[i, plane]
            for offset, w in operands:
                part = folded(v * w)
                target[offset + i] = part if fresh else target[offset + i] + part

        fours = (count - first) // 4

        def four(t, carry):
            for q in range(4):
                one(first + 4 * t + q)
            return carry

        lax.fori_loop(0, fours, four, 0)
        for i in range(first + 4 * fours, count):
            one(i)

    def diagonal(shape):
        return lax.broadcasted_iota(jnp.int32, shape, 0) == lax.broadcasted_iota(
            jnp.int32, shape, 1
        )

    def as_row(column, count):
        return jnp.sum(
            jnp.where(diagonal((count, 128)), column, 0.0), axis=0, keepdims=True
        )

    def as_column(row):
        return jnp.sum(
            jnp.where(diagonal((ROWS, 128)), row, 0.0), axis=1, keepdims=True
        )

    def packed(ref, start, count):
        flat = jnp.sum(ref[start : start + count], axis=1)
        return as_row(jnp.sum(flat, axis=1, keepdims=True), count)

    def send_row(n, row):
        row_src[n] = row
        row_all[n, me] = row
        for place in partners(True):
            pltpu.make_async_remote_copy(
                row_src.at[n],
                row_all.at[n, me],
                row_send.at[n],
                row_recv.at[n],
                device_id=device(place),
                device_id_type=MESH,
            ).start()

    def row_bytes(n, sem):
        part = row_all.at[n, pl.ds(0, DEVICES - 1)]
        return pltpu.make_async_copy(part, part, sem.at[n])

    def get_row(n):
        row_bytes(n, row_recv).wait()
        return jnp.sum(row_all[n], axis=0) * inv_cells

    row_id = lax.broadcasted_iota(jnp.int32, (ROWS, 128), 0)
    lane_id = lax.broadcasted_iota(jnp.int32, (ROWS, 128), 1)
    lane_row = lax.broadcasted_iota(jnp.int32, (1, 128), 1)
    row_column = lax.broadcasted_iota(jnp.int32, (ROWS, 1), 0)

    loads[0].wait()
    for copy in loads[2:]:
        copy.wait()
    for plane in range(planes):
        project([(ROWS, V[last, plane])], plane, acc, 0, keep, plane == 0)
    pl.semaphore_wait(barrier, DEVICES - 1)
    for plane in order:
        send_plane(0, plane)

    block = 32
    size = block * 8
    tall = keep * 8

    def gram_tile(tile, carry):
        start = pl.multiple_of(tile * 8, 8)
        v = jnp.concatenate(
            [
                V[0:keep, plane, pl.ds(start, 8), :].reshape(tall, cols)
                for plane in range(planes)
            ],
            axis=1,
        )
        high = v.astype(jnp.bfloat16)
        rest = v - high.astype(f32)
        low = rest.astype(jnp.bfloat16)

        def product(a, b):
            return lax.dot_general(
                a, b, (((1,), (1,)), ((), ())), preferred_element_type=f32
            )

        gram_hh[...] += product(high, high[0:size])
        gram_hl[...] += product(high, low[0:size])
        gram_lh[...] += product(low[size:], high[0:size])
        square = rest[0:size] * rest[0:size]
        parts = [square[:, 128 * n : 128 * n + 128] for n in range(planes * cols // 128)]
        while len(parts) > 1:
            parts = [a + b for a, b in zip(parts[::2], parts[1::2])]
        gram_ll[...] += parts[0]
        return carry

    lax.fori_loop(0, rows // 8, gram_tile, 0)
    for plane in range(planes):
        project(
            [(ROWS * q, V[block + q, plane]) for q in range(3)],
            plane,
            acc_kept,
            block,
            last,
            plane == 0,
        )

    pick = (
        lax.div(lax.broadcasted_iota(jnp.int32, (size, 128), 0), 8)
        == lax.broadcasted_iota(jnp.int32, (size, 128), 1)
    ).astype(f32)

    def blocks(ref):
        count = ref.shape[0]
        same = lax.rem(
            lax.broadcasted_iota(jnp.int32, (count, size), 0), 8
        ) == lax.rem(lax.broadcasted_iota(jnp.int32, (count, size), 1), 8)
        kept = jnp.where(same, ref[...], 0.0).reshape(count // 8, 8, size)
        return jnp.dot(
            jnp.sum(kept, axis=1),
            pick,
            precision=lax.Precision.HIGHEST,
            preferred_element_type=f32,
        )

    hh, hl, lh = blocks(gram_hh), blocks(gram_hl), blocks(gram_lh)
    ll = jnp.sum(
        jnp.sum(gram_ll[...].reshape(block, 8, 128), axis=1), axis=1, keepdims=True
    )
    turned = jnp.concatenate([hl[0:block], jnp.zeros((96, 128), f32)], axis=0).T
    both = hh + hl
    square = both[0:block] + turned[0:block]
    square = square + jnp.where(diagonal((block, 128)), ll, 0.0)
    dense = square[0:8]
    for q in range(1, 4):
        dense = dense + pltpu.roll(square[8 * q : 8 * q + 8], block * q, 1)
    extra = jnp.zeros((1, 128), f32)
    for q in range(3):
        exact = packed(acc_kept, ROWS * q, ROWS)
        values = both[block + q : block + q + 1] + lh[q : q + 1]
        values = jnp.where(lane_row < block, values, exact)
        values = jnp.where(lane_row < keep, values, 0.0)
        extra = extra + (pltpu.roll(values, keep * q, 1) if q else values)
    pair_src[0:4] = dense[0:4]
    pair_src[4:5] = extra
    pair_src[5:8] = jnp.zeros((3, 128), f32)
    pair_src[8:12] = dense[4:8]
    pair_src[12:16] = jnp.zeros((4, 128), f32)
    theirs = pl.ds(pl.multiple_of((1 - core) * 8, 8), 8)
    partner = {"gy": 1 - core, "gx": chip}
    to_pair = pltpu.make_async_remote_copy(
        pair_src.at[theirs],
        pair_got,
        gram_send.at[0],
        gram_recv.at[0],
        device_id=partner,
        device_id_type=MESH,
    )
    to_pair.start()
    loads[1].wait()
    local_part(0)
    project([(0, W[2])], 2, acc, 0, keep, True)
    to_pair.wait_recv()
    mine = jnp.where(core == 0, pair_src[0:8], pair_src[8:16]) + pair_got[...]
    used = pl.ds(0, 5)
    half_src[...] = mine
    half_all[chip, 0:5] = mine[0:5]
    for place in partners(False):
        pltpu.make_async_remote_copy(
            half_src.at[used],
            half_all.at[chip, used],
            gram_send.at[1],
            gram_recv.at[1],
            device_id=device(place),
            device_id_type=MESH,
        ).start()

    def half_bytes(sem):
        part = half_all.at[pl.ds(0, CHIPS - 1), used]
        return pltpu.make_async_copy(part, part, sem.at[1])

    def finish_operator(step, count):
        s = WIND[0]
        high_plane(step)
        W[3] += high_x[step]
        project([(0, W[3])], 3, acc, 0, count, False)
        low_plane(step, planes - 1)
        W[1] -= (0.5 * s) * low_x[step, 1]
        project([(0, W[1])], 1, acc, 0, count, False)
        low_plane(step, planes - 2)
        W[0] += (1.0 + 2.0 * s) * low_x[step, 1] - (0.5 * s) * low_x[step, 0]
        project([(0, W[0])], 0, acc, 0, count, False)
        send_row(step, packed(acc, 0, 2 * ROWS))

    finish_operator(0, keep)

    half_bytes(gram_recv).wait()
    swap_buf[0] = jnp.sum(half_all[:, 0:5], axis=0) * inv_cells
    swap = pltpu.make_async_remote_copy(
        swap_buf.at[0],
        swap_buf.at[1],
        gram_send.at[2],
        gram_recv.at[2],
        device_id=partner,
        device_id_type=MESH,
    )
    swap.start()
    swap.wait_recv()
    even = jnp.where(core == 0, swap_buf[0], swap_buf[1])
    odd = jnp.where(core == 0, swap_buf[1], swap_buf[0])
    dense = jnp.concatenate([even[0:4], odd[0:4]], axis=0)
    parts = [dense] + [pltpu.roll(dense, 128 - block * q, 1) for q in range(1, 4)]
    square = jnp.concatenate(parts, axis=0)
    square = jnp.where(
        lax.broadcasted_iota(jnp.int32, (block, 128), 1) < block, square, 0.0
    )
    gram = jnp.concatenate([square, jnp.zeros((8, 128), f32)], axis=0)
    extra = even[4:5]
    values = [extra] + [pltpu.roll(extra, 128 - keep * q, 1) for q in range(1, 3)]
    for q in range(3):
        gram = jnp.where(row_id == block + q, values[q], gram)
    for q in range(3):
        gram = jnp.where(lane_id == block + q, as_column(values[q]), gram)
    eye = jnp.where(row_id == lane_id, 2.0, 0.0)
    lower = jnp.logical_and(row_id < last, lane_id < last)
    matrix = jnp.where(lower, eye - gram, 0.0)

    scale_row = jnp.ones((1, 128), f32)
    scale_column = jnp.ones((ROWS, 1), f32)
    results = jnp.zeros((ROWS, 128), f32)
    inverse = None
    for step in range(STEPS):
        count = keep + step
        if step > 0:
            local_part(step)
            project(
                [(0, W[2]), (ROWS, V[last + step, 2])], 2, acc, 0, count, True
            )
            for plane in (3, 1, 0):
                project([(ROWS, V[last + step, plane])], plane, acc, 0, count, False)
            if step > 1:
                for plane in range(planes):
                    out[step - 2, plane] = V[last + step - 1, plane] * inverse
            finish_operator(step, count)
        sums = get_row(step)
        if step > 0:
            square = jnp.sum(
                jnp.where(lane_row == ROWS + count - 1, sums, 0.0),
                axis=1,
                keepdims=True,
            )
            norm = jnp.sqrt(square + EPSILON)
            inverse = 1.0 / norm
            scale_row = jnp.where(lane_row == count - 1, inverse, scale_row)
            scale_column = jnp.where(row_column == count - 1, inverse, scale_column)
            results = jnp.where(
                jnp.logical_and(row_id == count - 1, lane_id == step - 1), norm, results
            )
            factor = scale_row * inverse
        else:
            factor = scale_row
        valid = lane_row < count
        first = jnp.where(valid, sums * factor, 0.0)
        cross = jnp.where(valid, pltpu.roll(sums, 128 - ROWS, 1) * factor, 0.0)
        cross_column = as_column(cross)
        matrix = jnp.where(row_id == count - 1, eye - cross, matrix)
        matrix = jnp.where(lane_id == count - 1, eye - cross_column, matrix)
        weights = jnp.sum(matrix * first, axis=1, keepdims=True)
        weights = jnp.where(row_column < count, weights, 0.0)
        results = jnp.where(lane_id == step, weights, results)
        hb[...] = jnp.broadcast_to(weights * scale_column, hb.shape)

        for plane in order:
            start = W[plane] if step == 0 else W[plane] * inverse

            def minus(i, total):
                return total - hb[pl.ds(i, 1), :] * V[i, plane]

            def four(t, total):
                for q in range(4):
                    total = minus(4 * t + q, total)
                return total

            total = lax.fori_loop(0, count // 4, four, start)
            for i in range(4 * (count // 4), count):
                total = minus(i, total)
            V[count, plane] = total
            if step + 1 < STEPS:
                send_plane(step + 1, plane)

    total = jnp.zeros((8, 128), f32)
    for plane in range(planes):
        v = V[keep + STEPS - 1, plane]
        total = total + folded(v * v)
    square = jnp.sum(jnp.sum(total, axis=0, keepdims=True), axis=1, keepdims=True)
    send_row(STEPS, jnp.broadcast_to(square, (1, 128)))
    for plane in range(planes):
        out[STEPS - 2, plane] = V[keep + STEPS - 2, plane] * inverse
    sums = get_row(STEPS)
    norm = jnp.sqrt(sums[:, 0:1] + EPSILON)
    inverse = 1.0 / norm
    results = jnp.where(
        jnp.logical_and(row_id == keep + STEPS - 1, lane_id == STEPS - 1), norm, results
    )
    hess[...] = results[:, 0:STEPS]
    for plane in range(planes):
        out[STEPS - 1, plane] = V[keep + STEPS - 1, plane] * inverse

    for step in range(STEPS):

        @pl.when(chip < CHIPS - 1)
        def _():
            to_next(step, planes - 2).wait_send()
            to_next(step, planes - 1).wait_send()

        @pl.when(chip > 0)
        def _():
            to_previous(step).wait_send()

        for plane in range(planes):
            to_side(step, plane).wait_send()
    for n in range(STEPS + 1):
        row_bytes(n, row_send).wait()
    to_pair.wait_send()
    half_bytes(gram_send).wait()
    swap.wait_send()


def body(basis_vectors, reaction):
    keep, planes, rows, cols = basis_vectors.shape
    f32 = jnp.float32
    field = (planes, rows, cols)
    dma = pltpu.SemaphoreType.DMA
    vmem = pltpu.VMEM
    return pl.pallas_call(
        functools.partial(kernel, keep, planes, rows, cols),
        out_shape=(
            jax.ShapeDtypeStruct((STEPS, *field), f32),
            jax.ShapeDtypeStruct((keep + STEPS, STEPS), f32),
        ),
        in_specs=[pl.BlockSpec(memory_space=pltpu.HBM)] * 2,
        out_specs=(
            pl.BlockSpec(memory_space=pltpu.VMEM),
            pl.BlockSpec(memory_space=pltpu.VMEM),
        ),
        scratch_shapes=[
            vmem((keep + STEPS, *field), f32),
            vmem(field, f32),
            vmem(field, f32),
            vmem((STEPS, 2, rows, cols), f32),
            vmem((STEPS, rows, cols), f32),
            vmem((STEPS, planes, 8, cols), f32),
            vmem((2 * ROWS, 8, 128), f32),
            vmem((3 * ROWS, 8, 128), f32),
            vmem((8 * keep, 256), f32),
            vmem((8 * keep, 256), f32),
            vmem((8 * keep - 256, 256), f32),
            vmem((256, 128), f32),
            vmem((ROWS, cols), f32),
            vmem((STEPS + 1, 1, 128), f32),
            vmem((STEPS + 1, DEVICES, 1, 128), f32),
            vmem((16, 128), f32),
            vmem((8, 128), f32),
            vmem((8, 128), f32),
            vmem((CHIPS, 8, 128), f32),
            vmem((2, 5, 128), f32),
            dma((9,)),
            dma((STEPS, 3)),
            dma((STEPS, 2)),
            dma((STEPS,)),
            dma((STEPS, planes)),
            dma((STEPS, planes)),
            dma((STEPS + 1,)),
            dma((STEPS + 1,)),
            dma((3,)),
            dma((3,)),
        ],
        compiler_params=pltpu.CompilerParams(
            collective_id=0,
            has_side_effects=True,
            vmem_limit_bytes=65890000,
        ),
    )(basis_vectors, reaction)


def solution(mesh):
    return jax.shard_map(
        body,
        mesh=mesh,
        in_specs=(P(None, "gx", "gy", None), P("gx", "gy", None)),
        out_specs=(P(None, "gx", "gy", None), P()),
        check_vma=False,
    )
```

```python
import functools

import jax
import jax.numpy as jnp
from jax import lax
from jax.experimental import pallas as pl
from jax.experimental.pallas import tpu as pltpu
from jax.sharding import PartitionSpec as P

MESH = pl.DeviceIdType.MESH
STEPS = 4
WIND = (0.9, 0.6, 0.4)
EPSILON = 1e-06
SIDE = 4
CHIPS = 64
DEVICES = 128
ROWS = 40


def hops(delta):
    return sum(min(d, SIDE - d) for d in delta[:3])


def partners(with_core):
    places = [
        (z, y, x, c)
        for z in range(SIDE)
        for y in range(SIDE)
        for x in range(SIDE)
        for c in range(2 if with_core else 1)
    ]
    return sorted(
        [p for p in places if any(p)], key=lambda p: (-hops(p), p[2], p[1], p[0])
    )


def kernel(
    keep,
    planes,
    rows,
    cols,
    basis,
    react,
    out,
    hess,
    V,
    W,
    RC,
    low_x,
    high_x,
    side_y,
    acc,
    acc_kept,
    gram_hh,
    gram_hl,
    gram_lh,
    gram_ll,
    hb,
    row_src,
    row_all,
    pair_src,
    pair_got,
    half_src,
    half_all,
    swap_buf,
    load_sem,
    x_send,
    low_recv,
    high_recv,
    y_send,
    y_recv,
    row_send,
    row_recv,
    gram_send,
    gram_recv,
):
    f32 = jnp.float32
    core = lax.axis_index("gy")
    chip = lax.axis_index("gx")
    me = core * CHIPS + chip
    cz, cy, cx = lax.div(chip, 16), lax.rem(lax.div(chip, 4), 4), lax.rem(chip, 4)
    zs = [lax.rem(cz + d, SIDE) * 16 for d in range(SIDE)]
    ys = [lax.rem(cy + d, SIDE) * 4 for d in range(SIDE)]
    xs = [lax.rem(cx + d, SIDE) for d in range(SIDE)]
    cores = [core, 1 - core]
    inv_cells = 1.0 / float(DEVICES * planes * rows * cols)

    def device(place):
        z, y, x, c = place
        return {"gy": cores[c], "gx": zs[z] + ys[y] + xs[x]}

    last = keep - 1
    loads = [
        pltpu.make_async_copy(basis.at[last], V.at[last], load_sem.at[0]),
        pltpu.make_async_copy(react, RC, load_sem.at[1]),
    ]
    for n, start in enumerate(range(0, last, 7)):
        part = pl.ds(start, min(7, last - start))
        loads.append(
            pltpu.make_async_copy(basis.at[part], V.at[part], load_sem.at[2 + n])
        )
    for copy in loads:
        copy.start()

    barrier = pltpu.get_barrier_semaphore()
    for place in partners(True):
        pl.semaphore_signal(
            barrier, inc=1, device_id=device(place), device_id_type=MESH
        )

    acc[...] = jnp.zeros(acc.shape, f32)
    acc_kept[...] = jnp.zeros(acc_kept.shape, f32)
    gram_hh[...] = jnp.zeros(gram_hh.shape, f32)
    gram_hl[...] = jnp.zeros(gram_hl.shape, f32)
    gram_lh[...] = jnp.zeros(gram_lh.shape, f32)
    gram_ll[...] = jnp.zeros(gram_ll.shape, f32)

    @pl.when(chip == 0)
    def _():
        low_x[...] = jnp.zeros(low_x.shape, f32)

    @pl.when(chip == CHIPS - 1)
    def _():
        high_x[...] = jnp.zeros(high_x.shape, f32)

    def to_next(step, plane):
        return pltpu.make_async_remote_copy(
            V.at[last + step, plane],
            low_x.at[step, plane - (planes - 2)],
            x_send.at[step, plane - (planes - 2)],
            low_recv.at[step, plane - (planes - 2)],
            device_id={"gy": core, "gx": lax.rem(chip + 1, CHIPS)},
            device_id_type=MESH,
        )

    def to_previous(step):
        return pltpu.make_async_remote_copy(
            V.at[last + step, 0],
            high_x.at[step],
            x_send.at[step, 2],
            high_recv.at[step],
            device_id={"gy": core, "gx": lax.rem(chip + CHIPS - 1, CHIPS)},
            device_id_type=MESH,
        )

    edge = pl.ds(pl.multiple_of((1 - core) * (rows - 8), 8), 8)

    def to_side(step, plane):
        return pltpu.make_async_remote_copy(
            V.at[last + step, plane, edge],
            side_y.at[step, plane],
            y_send.at[step, plane],
            y_recv.at[step, plane],
            device_id={"gy": 1 - core, "gx": chip},
            device_id_type=MESH,
        )

    def send_plane(step, plane):
        if plane >= planes - 2:

            @pl.when(chip < CHIPS - 1)
            def _():
                to_next(step, plane).start()

        if plane == 0:

            @pl.when(chip > 0)
            def _():
                to_previous(step).start()

        to_side(step, plane).start()

    order = (3, 2, 0, 1)

    lanes = lax.broadcasted_iota(jnp.int32, (rows, cols), 1)

    def local_part(step):
        centre = 6.0 + 1.5 * sum(WIND)
        index = last + step
        for plane in range(planes):
            to_side(step, plane).wait_recv()
        for plane in range(planes):
            v = V[index, plane]
            side = side_y[step, plane]
            below = jnp.where(core == 1, side, 0.0)
            above = jnp.where(core == 0, side, 0.0)
            tall = jnp.concatenate([below, v, above], axis=0)
            total = -(RC[plane] + centre) * v
            s = WIND[1]
            total += tall[9 : rows + 9]
            total += (1.0 + 2.0 * s) * tall[7 : rows + 7] - (0.5 * s) * tall[6 : rows + 6]
            s = WIND[2]
            total += jnp.where(lanes < cols - 1, pltpu.roll(v, cols - 1, 1), 0.0)
            total += (1.0 + 2.0 * s) * jnp.where(lanes >= 1, pltpu.roll(v, 1, 1), 0.0)
            total -= (0.5 * s) * jnp.where(lanes >= 2, pltpu.roll(v, 2, 1), 0.0)
            s = WIND[0]
            if plane + 1 < planes:
                total += V[index, plane + 1]
            if plane >= 1:
                total += (1.0 + 2.0 * s) * V[index, plane - 1]
            if plane >= 2:
                total -= (0.5 * s) * V[index, plane - 2]
            W[plane] = total

    def low_plane(step, plane):
        @pl.when(chip > 0)
        def _():
            to_next(step, plane).wait_recv()

    def high_plane(step):
        @pl.when(chip < CHIPS - 1)
        def _():
            to_previous(step).wait_recv()

    def folded(product):
        half = product[:, : cols // 2] + product[:, cols // 2 :]
        parts = [half[8 * t : 8 * t + 8] for t in range(rows // 8)]
        while len(parts) > 1:
            parts = [a + b for a, b in zip(parts[::2], parts[1::2])]
        return parts[0]

    def project(operands, plane, target, first, count, fresh):
        def one(i):
            v = V[i, plane]
            for offset, w in operands:
                part = folded(v * w)
                target[offset + i] = part if fresh else target[offset + i] + part

        fours = (count - first) // 4

        def four(t, carry):
            for q in range(4):
                one(first + 4 * t + q)
            return carry

        lax.fori_loop(0, fours, four, 0)
        for i in range(first + 4 * fours, count):
            one(i)

    def diagonal(shape):
        return lax.broadcasted_iota(jnp.int32, shape, 0) == lax.broadcasted_iota(
            jnp.int32, shape, 1
        )

    def as_row(column, count):
        return jnp.sum(
            jnp.where(diagonal((count, 128)), column, 0.0), axis=0, keepdims=True
        )

    def as_column(row):
        return jnp.sum(
            jnp.where(diagonal((ROWS, 128)), row, 0.0), axis=1, keepdims=True
        )

    def packed(ref, start, count):
        flat = jnp.sum(ref[start : start + count], axis=1)
        return as_row(jnp.sum(flat, axis=1, keepdims=True), count)

    def send_row(n, row):
        row_src[n] = row
        row_all[n, me] = row
        for place in partners(True):
            pltpu.make_async_remote_copy(
                row_src.at[n],
                row_all.at[n, me],
                row_send.at[n],
                row_recv.at[n],
                device_id=device(place),
                device_id_type=MESH,
            ).start()

    def row_bytes(n, sem):
        part = row_all.at[n, pl.ds(0, DEVICES - 1)]
        return pltpu.make_async_copy(part, part, sem.at[n])

    def get_row(n):
        row_bytes(n, row_recv).wait()
        return jnp.sum(row_all[n], axis=0) * inv_cells

    row_id = lax.broadcasted_iota(jnp.int32, (ROWS, 128), 0)
    lane_id = lax.broadcasted_iota(jnp.int32, (ROWS, 128), 1)
    lane_row = lax.broadcasted_iota(jnp.int32, (1, 128), 1)
    row_column = lax.broadcasted_iota(jnp.int32, (ROWS, 1), 0)

    loads[0].wait()
    for copy in loads[2:]:
        copy.wait()
    for plane in range(planes):
        project([(ROWS, V[last, plane])], plane, acc, 0, keep, plane == 0)
    pl.semaphore_wait(barrier, DEVICES - 1)
    for plane in order:
        send_plane(0, plane)

    block = 32
    size = block * 8
    tall = keep * 8

    def gram_tile(tile, carry):
        start = pl.multiple_of(tile * 8, 8)
        v = jnp.concatenate(
            [
                V[0:keep, plane, pl.ds(start, 8), :].reshape(tall, cols)
                for plane in range(planes)
            ],
            axis=1,
        )
        high = v.astype(jnp.bfloat16)
        rest = v - high.astype(f32)
        low = rest.astype(jnp.bfloat16)

        def product(a, b):
            return lax.dot_general(
                a, b, (((1,), (1,)), ((), ())), preferred_element_type=f32
            )

        gram_hh[...] += product(high, high[0:size])
        gram_hl[...] += product(high, low[0:size])
        gram_lh[...] += product(low[size:], high[0:size])
        square = rest[0:size] * rest[0:size]
        parts = [square[:, 128 * n : 128 * n + 128] for n in range(planes * cols // 128)]
        while len(parts) > 1:
            parts = [a + b for a, b in zip(parts[::2], parts[1::2])]
        gram_ll[...] += parts[0]
        return carry

    lax.fori_loop(0, rows // 8, gram_tile, 0)
    for plane in range(planes):
        project(
            [(ROWS * q, V[block + q, plane]) for q in range(3)],
            plane,
            acc_kept,
            block,
            last,
            plane == 0,
        )

    pick = (
        lax.div(lax.broadcasted_iota(jnp.int32, (size, 128), 0), 8)
        == lax.broadcasted_iota(jnp.int32, (size, 128), 1)
    ).astype(f32)

    def blocks(ref):
        count = ref.shape[0]
        same = lax.rem(
            lax.broadcasted_iota(jnp.int32, (count, size), 0), 8
        ) == lax.rem(lax.broadcasted_iota(jnp.int32, (count, size), 1), 8)
        kept = jnp.where(same, ref[...], 0.0).reshape(count // 8, 8, size)
        return jnp.dot(
            jnp.sum(kept, axis=1),
            pick,
            precision=lax.Precision.HIGHEST,
            preferred_element_type=f32,
        )

    hh, hl, lh = blocks(gram_hh), blocks(gram_hl), blocks(gram_lh)
    ll = jnp.sum(
        jnp.sum(gram_ll[...].reshape(block, 8, 128), axis=1), axis=1, keepdims=True
    )
    turned = jnp.concatenate([hl[0:block], jnp.zeros((96, 128), f32)], axis=0).T
    both = hh + hl
    square = both[0:block] + turned[0:block]
    square = square + jnp.where(diagonal((block, 128)), ll, 0.0)
    dense = square[0:8]
    for q in range(1, 4):
        dense = dense + pltpu.roll(square[8 * q : 8 * q + 8], block * q, 1)
    extra = jnp.zeros((1, 128), f32)
    for q in range(3):
        exact = packed(acc_kept, ROWS * q, ROWS)
        values = both[block + q : block + q + 1] + lh[q : q + 1]
        values = jnp.where(lane_row < block, values, exact)
        values = jnp.where(lane_row < keep, values, 0.0)
        extra = extra + (pltpu.roll(values, keep * q, 1) if q else values)
    pair_src[0:4] = dense[0:4]
    pair_src[4:5] = extra
    pair_src[5:8] = jnp.zeros((3, 128), f32)
    pair_src[8:12] = dense[4:8]
    pair_src[12:16] = jnp.zeros((4, 128), f32)
    theirs = pl.ds(pl.multiple_of((1 - core) * 8, 8), 8)
    partner = {"gy": 1 - core, "gx": chip}
    to_pair = pltpu.make_async_remote_copy(
        pair_src.at[theirs],
        pair_got,
        gram_send.at[0],
        gram_recv.at[0],
        device_id=partner,
        device_id_type=MESH,
    )
    to_pair.start()
    loads[1].wait()
    local_part(0)
    project([(0, W[2])], 2, acc, 0, keep, True)
    to_pair.wait_recv()
    mine = jnp.where(core == 0, pair_src[0:8], pair_src[8:16]) + pair_got[...]
    used = pl.ds(0, 5)
    half_src[...] = mine
    half_all[chip, 0:5] = mine[0:5]
    for place in partners(False):
        pltpu.make_async_remote_copy(
            half_src.at[used],
            half_all.at[chip, used],
            gram_send.at[1],
            gram_recv.at[1],
            device_id=device(place),
            device_id_type=MESH,
        ).start()

    def half_bytes(sem):
        part = half_all.at[pl.ds(0, CHIPS - 1), used]
        return pltpu.make_async_copy(part, part, sem.at[1])

    def finish_operator(step, count):
        s = WIND[0]
        high_plane(step)
        W[3] += high_x[step]
        project([(0, W[3])], 3, acc, 0, count, False)
        low_plane(step, planes - 1)
        W[1] -= (0.5 * s) * low_x[step, 1]
        project([(0, W[1])], 1, acc, 0, count, False)
        low_plane(step, planes - 2)
        W[0] += (1.0 + 2.0 * s) * low_x[step, 1] - (0.5 * s) * low_x[step, 0]
        project([(0, W[0])], 0, acc, 0, count, False)
        send_row(step, packed(acc, 0, 2 * ROWS))

    finish_operator(0, keep)

    half_bytes(gram_recv).wait()
    swap_buf[0] = jnp.sum(half_all[:, 0:5], axis=0) * inv_cells
    swap = pltpu.make_async_remote_copy(
        swap_buf.at[0],
        swap_buf.at[1],
        gram_send.at[2],
        gram_recv.at[2],
        device_id=partner,
        device_id_type=MESH,
    )
    swap.start()
    swap.wait_recv()
    even = jnp.where(core == 0, swap_buf[0], swap_buf[1])
    odd = jnp.where(core == 0, swap_buf[1], swap_buf[0])
    dense = jnp.concatenate([even[0:4], odd[0:4]], axis=0)
    parts = [dense] + [pltpu.roll(dense, 128 - block * q, 1) for q in range(1, 4)]
    square = jnp.concatenate(parts, axis=0)
    square = jnp.where(
        lax.broadcasted_iota(jnp.int32, (block, 128), 1) < block, square, 0.0
    )
    gram = jnp.concatenate([square, jnp.zeros((8, 128), f32)], axis=0)
    extra = even[4:5]
    values = [extra] + [pltpu.roll(extra, 128 - keep * q, 1) for q in range(1, 3)]
    for q in range(3):
        gram = jnp.where(row_id == block + q, values[q], gram)
    for q in range(3):
        gram = jnp.where(lane_id == block + q, as_column(values[q]), gram)
    eye = jnp.where(row_id == lane_id, 2.0, 0.0)
    lower = jnp.logical_and(row_id < last, lane_id < last)
    matrix = jnp.where(lower, eye - gram, 0.0)

    scale_row = jnp.ones((1, 128), f32)
    scale_column = jnp.ones((ROWS, 1), f32)
    results = jnp.zeros((8, 128), f32)
    row_8 = lax.broadcasted_iota(jnp.int32, (8, 128), 0)
    lane_8 = lax.broadcasted_iota(jnp.int32, (8, 128), 1)
    inverse = None
    for step in range(STEPS):
        count = keep + step
        if step > 0:
            local_part(step)
            project(
                [(0, W[2]), (ROWS, V[last + step, 2])], 2, acc, 0, count, True
            )
            for plane in (3, 1, 0):
                project([(ROWS, V[last + step, plane])], plane, acc, 0, count, False)
            if step > 1:
                for plane in range(planes):
                    out[step - 2, plane] = V[last + step - 1, plane] * inverse
            finish_operator(step, count)
        sums = get_row(step)
        if step > 0:
            square = jnp.sum(
                jnp.where(lane_row == ROWS + count - 1, sums, 0.0),
                axis=1,
                keepdims=True,
            )
            norm = jnp.sqrt(square + EPSILON)
            inverse = 1.0 / norm
            scale_row = jnp.where(lane_row == count - 1, inverse, scale_row)
            scale_column = jnp.where(row_column == count - 1, inverse, scale_column)
            results = jnp.where(
                jnp.logical_and(row_8 == step - 1, lane_8 == count - 1), norm, results
            )
            factor = scale_row * inverse
        else:
            factor = scale_row
        valid = lane_row < count
        first = jnp.where(valid, sums * factor, 0.0)
        cross = jnp.where(valid, pltpu.roll(sums, 128 - ROWS, 1) * factor, 0.0)
        cross_column = as_column(cross)
        matrix = jnp.where(row_id == count - 1, eye - cross, matrix)
        matrix = jnp.where(lane_id == count - 1, eye - cross_column, matrix)
        weights = jnp.sum(matrix * first, axis=1, keepdims=True)
        weights = jnp.where(row_column < count, weights, 0.0)
        hb[...] = jnp.broadcast_to(weights * scale_column, hb.shape)

        for plane in order:
            start = W[plane] if step == 0 else W[plane] * inverse

            def minus(i, total):
                return total - hb[pl.ds(i, 1), :] * V[i, plane]

            def four(t, total):
                for q in range(4):
                    total = minus(4 * t + q, total)
                return total

            total = lax.fori_loop(0, count // 4, four, start)
            for i in range(4 * (count // 4), count):
                total = minus(i, total)
            V[count, plane] = total
            if step + 1 < STEPS:
                send_plane(step + 1, plane)
        results = jnp.where(row_8 == step, as_row(weights, ROWS), results)

    total = jnp.zeros((8, 128), f32)
    for plane in range(planes):
        v = V[keep + STEPS - 1, plane]
        total = total + folded(v * v)
    square = jnp.sum(jnp.sum(total, axis=0, keepdims=True), axis=1, keepdims=True)
    send_row(STEPS, jnp.broadcast_to(square, (1, 128)))
    for plane in range(planes):
        out[STEPS - 2, plane] = V[keep + STEPS - 2, plane] * inverse
    sums = get_row(STEPS)
    norm = jnp.sqrt(sums[:, 0:1] + EPSILON)
    inverse = 1.0 / norm
    results = jnp.where(
        jnp.logical_and(row_8 == STEPS - 1, lane_8 == keep + STEPS - 1), norm, results
    )
    hess[...] = results[0:STEPS, 0:ROWS]
    for plane in range(planes):
        out[STEPS - 1, plane] = V[keep + STEPS - 1, plane] * inverse

    for step in range(STEPS):

        @pl.when(chip < CHIPS - 1)
        def _():
            to_next(step, planes - 2).wait_send()
            to_next(step, planes - 1).wait_send()

        @pl.when(chip > 0)
        def _():
            to_previous(step).wait_send()

        for plane in range(planes):
            to_side(step, plane).wait_send()
    for n in range(STEPS + 1):
        row_bytes(n, row_send).wait()
    to_pair.wait_send()
    half_bytes(gram_send).wait()
    swap.wait_send()


def put_out(vectors, columns, vectors_out, columns_out, sem):
    copies = [
        pltpu.make_async_copy(vectors, vectors_out, sem.at[0]),
        pltpu.make_async_copy(columns, columns_out, sem.at[1]),
    ]
    for copy in copies:
        copy.start()
    for copy in copies:
        copy.wait()


def body(basis_vectors, reaction):
    keep, planes, rows, cols = basis_vectors.shape
    f32 = jnp.float32
    field = (planes, rows, cols)
    dma = pltpu.SemaphoreType.DMA
    vmem = pltpu.VMEM
    reaction = pltpu.with_memory_space_constraint(reaction, pltpu.HBM)
    vectors, columns = pl.pallas_call(
        functools.partial(kernel, keep, planes, rows, cols),
        out_shape=(
            jax.ShapeDtypeStruct((STEPS, *field), f32),
            jax.ShapeDtypeStruct((STEPS, keep + STEPS), f32),
        ),
        in_specs=[pl.BlockSpec(memory_space=pltpu.HBM)] * 2,
        out_specs=(
            pl.BlockSpec(memory_space=pltpu.VMEM),
            pl.BlockSpec(memory_space=pltpu.VMEM),
        ),
        scratch_shapes=[
            vmem((keep + STEPS, *field), f32),
            vmem(field, f32),
            vmem(field, f32),
            vmem((STEPS, 2, rows, cols), f32),
            vmem((STEPS, rows, cols), f32),
            vmem((STEPS, planes, 8, cols), f32),
            vmem((2 * ROWS, 8, 128), f32),
            vmem((3 * ROWS, 8, 128), f32),
            vmem((8 * keep, 256), f32),
            vmem((8 * keep, 256), f32),
            vmem((8 * keep - 256, 256), f32),
            vmem((256, 128), f32),
            vmem((ROWS, cols), f32),
            vmem((STEPS + 1, 1, 128), f32),
            vmem((STEPS + 1, DEVICES, 1, 128), f32),
            vmem((16, 128), f32),
            vmem((8, 128), f32),
            vmem((8, 128), f32),
            vmem((CHIPS, 8, 128), f32),
            vmem((2, 5, 128), f32),
            dma((9,)),
            dma((STEPS, 3)),
            dma((STEPS, 2)),
            dma((STEPS,)),
            dma((STEPS, planes)),
            dma((STEPS, planes)),
            dma((STEPS + 1,)),
            dma((STEPS + 1,)),
            dma((3,)),
            dma((3,)),
        ],
        compiler_params=pltpu.CompilerParams(
            collective_id=0,
            has_side_effects=True,
            vmem_limit_bytes=48 * 1024 * 1024,
        ),
    )(basis_vectors, reaction)
    shapes = (vectors, columns)
    new_vectors, rows_out = pl.pallas_call(
        put_out,
        out_shape=tuple(jax.ShapeDtypeStruct(a.shape, f32) for a in shapes),
        in_specs=[pl.BlockSpec(memory_space=pltpu.VMEM)] * 2,
        out_specs=(pl.BlockSpec(memory_space=pl.ANY),) * 2,
        scratch_shapes=[dma((2,))],
        compiler_params=pltpu.CompilerParams(vmem_limit_bytes=4 * 1024 * 1024),
    )(vectors, columns)
    return new_vectors, rows_out.T


def solution(mesh):
    return jax.shard_map(
        body,
        mesh=mesh,
        in_specs=(P(None, "gx", "gy", None), P("gx", "gy", None)),
        out_specs=(P(None, "gx", "gy", None), P()),
        check_vma=False,
    )
```

```python
import functools

import jax
import jax.numpy as jnp
from jax import lax
from jax.experimental import pallas as pl
from jax.experimental.pallas import tpu as pltpu
from jax.sharding import PartitionSpec as P

MESH = pl.DeviceIdType.MESH
STEPS = 4
WIND = (0.9, 0.6, 0.4)
EPSILON = 1e-06
SIDE = 4
CHIPS = 64
DEVICES = 128
ROWS = 40
PIECES = {2: 4, 3: 2}


def hops(delta):
    return sum(min(d, SIDE - d) for d in delta[:3])


def partners(with_core):
    places = [
        (z, y, x, c)
        for z in range(SIDE)
        for y in range(SIDE)
        for x in range(SIDE)
        for c in range(2 if with_core else 1)
    ]
    return sorted(
        [p for p in places if any(p)], key=lambda p: (-hops(p), p[2], p[1], p[0])
    )


def kernel(
    keep,
    planes,
    rows,
    cols,
    basis,
    react,
    out,
    hess,
    V,
    W,
    RC,
    low_x,
    high_x,
    side_y,
    acc,
    acc_kept,
    gram_hh,
    gram_hl,
    gram_lh,
    gram_ll,
    hb,
    row_src,
    row_all,
    pair_src,
    pair_got,
    half_src,
    half_all,
    swap_buf,
    load_sem,
    next_send,
    x_send,
    low_recv,
    high_recv,
    y_send,
    y_recv,
    row_send,
    row_recv,
    gram_send,
    gram_recv,
):
    f32 = jnp.float32
    core = lax.axis_index("gy")
    chip = lax.axis_index("gx")
    me = core * CHIPS + chip
    cz, cy, cx = lax.div(chip, 16), lax.rem(lax.div(chip, 4), 4), lax.rem(chip, 4)
    zs = [lax.rem(cz + d, SIDE) * 16 for d in range(SIDE)]
    ys = [lax.rem(cy + d, SIDE) * 4 for d in range(SIDE)]
    xs = [lax.rem(cx + d, SIDE) for d in range(SIDE)]
    cores = [core, 1 - core]
    inv_cells = 1.0 / float(DEVICES * planes * rows * cols)

    def device(place):
        z, y, x, c = place
        return {"gy": cores[c], "gx": zs[z] + ys[y] + xs[x]}

    last = keep - 1
    loads = [
        pltpu.make_async_copy(basis.at[last], V.at[last], load_sem.at[0]),
        pltpu.make_async_copy(react, RC, load_sem.at[1]),
    ]
    for n, start in enumerate(range(0, last, 7)):
        part = pl.ds(start, min(7, last - start))
        loads.append(
            pltpu.make_async_copy(basis.at[part], V.at[part], load_sem.at[2 + n])
        )
    for copy in loads:
        copy.start()

    barrier = pltpu.get_barrier_semaphore()
    for place in partners(True):
        pl.semaphore_signal(
            barrier, inc=1, device_id=device(place), device_id_type=MESH
        )

    acc[...] = jnp.zeros(acc.shape, f32)
    acc_kept[...] = jnp.zeros(acc_kept.shape, f32)
    gram_hh[...] = jnp.zeros(gram_hh.shape, f32)
    gram_hl[...] = jnp.zeros(gram_hl.shape, f32)
    gram_lh[...] = jnp.zeros(gram_lh.shape, f32)
    gram_ll[...] = jnp.zeros(gram_ll.shape, f32)

    @pl.when(chip == 0)
    def _():
        low_x[...] = jnp.zeros(low_x.shape, f32)

    @pl.when(chip == CHIPS - 1)
    def _():
        high_x[...] = jnp.zeros(high_x.shape, f32)

    def piece(plane, part):
        size = rows // PIECES[plane]
        return pl.ds(part * size, size)

    def to_next(step, plane, part):
        place, where = plane - (planes - 2), piece(plane, part)
        return pltpu.make_async_remote_copy(
            V.at[last + step, plane, where],
            low_x.at[step, place, where],
            next_send.at[step, place, part],
            low_recv.at[step, place, part],
            device_id={"gy": core, "gx": lax.rem(chip + 1, CHIPS)},
            device_id_type=MESH,
        )

    def to_previous(step):
        return pltpu.make_async_remote_copy(
            V.at[last + step, 0],
            high_x.at[step],
            x_send.at[step],
            high_recv.at[step],
            device_id={"gy": core, "gx": lax.rem(chip + CHIPS - 1, CHIPS)},
            device_id_type=MESH,
        )

    edge = pl.ds(pl.multiple_of((1 - core) * (rows - 8), 8), 8)

    def to_side(step, plane):
        return pltpu.make_async_remote_copy(
            V.at[last + step, plane, edge],
            side_y.at[step, plane],
            y_send.at[step, plane],
            y_recv.at[step, plane],
            device_id={"gy": 1 - core, "gx": chip},
            device_id_type=MESH,
        )

    def send_piece(step, plane, part):
        @pl.when(chip < CHIPS - 1)
        def _():
            to_next(step, plane, part).start()

    def send_rest(step, plane):
        if plane == 0:

            @pl.when(chip > 0)
            def _():
                to_previous(step).start()

        to_side(step, plane).start()

    def send_plane(step, plane):
        if plane >= planes - 2:
            for part in range(PIECES[plane]):
                send_piece(step, plane, part)
        send_rest(step, plane)

    order = (3, 0, 2, 1)

    lanes = lax.broadcasted_iota(jnp.int32, (rows, cols), 1)

    def local_part(step):
        centre = 6.0 + 1.5 * sum(WIND)
        index = last + step
        for plane in range(planes):
            to_side(step, plane).wait_recv()
        for plane in range(planes):
            v = V[index, plane]
            side = side_y[step, plane]
            below = jnp.where(core == 1, side, 0.0)
            above = jnp.where(core == 0, side, 0.0)
            tall = jnp.concatenate([below, v, above], axis=0)
            total = -(RC[plane] + centre) * v
            s = WIND[1]
            total += tall[9 : rows + 9]
            total += (1.0 + 2.0 * s) * tall[7 : rows + 7] - (0.5 * s) * tall[6 : rows + 6]
            s = WIND[2]
            total += jnp.where(lanes < cols - 1, pltpu.roll(v, cols - 1, 1), 0.0)
            total += (1.0 + 2.0 * s) * jnp.where(lanes >= 1, pltpu.roll(v, 1, 1), 0.0)
            total -= (0.5 * s) * jnp.where(lanes >= 2, pltpu.roll(v, 2, 1), 0.0)
            s = WIND[0]
            if plane + 1 < planes:
                total += V[index, plane + 1]
            if plane >= 1:
                total += (1.0 + 2.0 * s) * V[index, plane - 1]
            if plane >= 2:
                total -= (0.5 * s) * V[index, plane - 2]
            W[plane] = total

    def low_plane(step, plane, part):
        @pl.when(chip > 0)
        def _():
            to_next(step, plane, part).wait_recv()

    def high_plane(step):
        @pl.when(chip < CHIPS - 1)
        def _():
            to_previous(step).wait_recv()

    def folded(product):
        half = product[:, : cols // 2] + product[:, cols // 2 :]
        parts = [half[8 * t : 8 * t + 8] for t in range(product.shape[0] // 8)]
        while len(parts) > 1:
            parts = [a + b for a, b in zip(parts[::2], parts[1::2])]
        return parts[0]

    def project(operands, plane, target, first, count, fresh, where=slice(None)):
        def one(i):
            v = V[i, plane, where]
            for offset, w in operands:
                part = folded(v * w)
                target[offset + i] = part if fresh else target[offset + i] + part

        fours = (count - first) // 4

        def four(t, carry):
            for q in range(4):
                one(first + 4 * t + q)
            return carry

        lax.fori_loop(0, fours, four, 0)
        for i in range(first + 4 * fours, count):
            one(i)

    def diagonal(shape):
        return lax.broadcasted_iota(jnp.int32, shape, 0) == lax.broadcasted_iota(
            jnp.int32, shape, 1
        )

    def as_row(column, count):
        return jnp.sum(
            jnp.where(diagonal((count, 128)), column, 0.0), axis=0, keepdims=True
        )

    def as_column(row):
        return jnp.sum(
            jnp.where(diagonal((ROWS, 128)), row, 0.0), axis=1, keepdims=True
        )

    def packed(ref, start, count):
        flat = jnp.sum(ref[start : start + count], axis=1)
        return as_row(jnp.sum(flat, axis=1, keepdims=True), count)

    def send_row(n, row):
        row_src[n] = row
        row_all[n, me] = row
        for place in partners(True):
            pltpu.make_async_remote_copy(
                row_src.at[n],
                row_all.at[n, me],
                row_send.at[n],
                row_recv.at[n],
                device_id=device(place),
                device_id_type=MESH,
            ).start()

    def row_bytes(n, sem):
        part = row_all.at[n, pl.ds(0, DEVICES - 1)]
        return pltpu.make_async_copy(part, part, sem.at[n])

    def get_row(n):
        row_bytes(n, row_recv).wait()
        return jnp.sum(row_all[n], axis=0) * inv_cells

    row_id = lax.broadcasted_iota(jnp.int32, (ROWS, 128), 0)
    lane_id = lax.broadcasted_iota(jnp.int32, (ROWS, 128), 1)
    lane_row = lax.broadcasted_iota(jnp.int32, (1, 128), 1)
    row_column = lax.broadcasted_iota(jnp.int32, (ROWS, 1), 0)

    loads[0].wait()
    for copy in loads[2:]:
        copy.wait()
    block = 32
    size = block * 8
    tall = keep * 8

    def gram_tile(tile, carry):
        start = pl.multiple_of(tile * 8, 8)
        v = jnp.concatenate(
            [
                V[0:keep, plane, pl.ds(start, 8), :].reshape(tall, cols)
                for plane in range(planes)
            ],
            axis=1,
        )
        high = v.astype(jnp.bfloat16)
        rest = v - high.astype(f32)
        low = rest.astype(jnp.bfloat16)

        def product(a, b):
            return lax.dot_general(
                a, b, (((1,), (1,)), ((), ())), preferred_element_type=f32
            )

        gram_hh[...] += product(high, high[0:size])
        gram_hl[...] += product(high, low[0:size])
        gram_lh[...] += product(low[size:], high[0:size])
        square = rest[0:size] * rest[0:size]
        parts = [square[:, 128 * n : 128 * n + 128] for n in range(planes * cols // 128)]
        while len(parts) > 1:
            parts = [a + b for a, b in zip(parts[::2], parts[1::2])]
        gram_ll[...] += parts[0]
        return carry

    early = 2
    lax.fori_loop(0, early, gram_tile, 0)
    pl.semaphore_wait(barrier, DEVICES - 1)
    for plane in order:
        send_plane(0, plane)
    lax.fori_loop(early, rows // 8, gram_tile, 0)
    for plane in range(planes):
        project(
            [(ROWS * q, V[block + q, plane]) for q in range(3)],
            plane,
            acc_kept,
            block,
            last,
            plane == 0,
        )

    pick = (
        lax.div(lax.broadcasted_iota(jnp.int32, (size, 128), 0), 8)
        == lax.broadcasted_iota(jnp.int32, (size, 128), 1)
    ).astype(f32)

    def blocks(matrix):
        count = matrix.shape[0]
        same = lax.rem(
            lax.broadcasted_iota(jnp.int32, (count, size), 0), 8
        ) == lax.rem(lax.broadcasted_iota(jnp.int32, (count, size), 1), 8)
        kept = jnp.where(same, matrix, 0.0).reshape(count // 8, 8, size)
        return jnp.sum(kept, axis=1)

    stacked = jnp.concatenate(
        [
            blocks(0.5 * gram_hh[0:size] + gram_hl[0:size]),
            blocks(gram_hh[size:] + gram_hl[size:] + gram_lh[...]),
        ],
        axis=0,
    )
    inner = jnp.dot(
        stacked, pick, precision=lax.Precision.HIGHEST, preferred_element_type=f32
    )
    ll = jnp.sum(
        jnp.sum(gram_ll[...].reshape(block, 8, 128), axis=1), axis=1, keepdims=True
    )
    turned = jnp.concatenate([inner[0:block], jnp.zeros((96, 128), f32)], axis=0).T
    square = inner[0:block] + turned[0:block]
    square = square + jnp.where(diagonal((block, 128)), ll, 0.0)
    dense = square[0:8]
    for q in range(1, 4):
        dense = dense + pltpu.roll(square[8 * q : 8 * q + 8], block * q, 1)
    extra = jnp.zeros((1, 128), f32)
    for q in range(3):
        exact = packed(acc_kept, ROWS * q, ROWS)
        values = inner[block + q : block + q + 1]
        values = jnp.where(lane_row < block, values, exact)
        values = jnp.where(lane_row < keep, values, 0.0)
        extra = extra + (pltpu.roll(values, keep * q, 1) if q else values)
    pair_src[0:4] = dense[0:4]
    pair_src[4:5] = extra
    pair_src[5:8] = jnp.zeros((3, 128), f32)
    pair_src[8:12] = dense[4:8]
    pair_src[12:16] = jnp.zeros((4, 128), f32)
    theirs = pl.ds(pl.multiple_of((1 - core) * 8, 8), 8)
    partner = {"gy": 1 - core, "gx": chip}
    to_pair = pltpu.make_async_remote_copy(
        pair_src.at[theirs],
        pair_got,
        gram_send.at[0],
        gram_recv.at[0],
        device_id=partner,
        device_id_type=MESH,
    )
    to_pair.start()
    loads[1].wait()
    local_part(0)
    project([(0, W[2]), (ROWS, V[last, 2])], 2, acc, 0, keep, True)
    to_pair.wait_recv()
    mine = jnp.where(core == 0, pair_src[0:8], pair_src[8:16]) + pair_got[...]
    used = pl.ds(0, 5)
    half_src[...] = mine
    half_all[chip, 0:5] = mine[0:5]
    for place in partners(False):
        pltpu.make_async_remote_copy(
            half_src.at[used],
            half_all.at[chip, used],
            gram_send.at[1],
            gram_recv.at[1],
            device_id=device(place),
            device_id_type=MESH,
        ).start()

    for plane in (3, 1, 0):
        project([(ROWS, V[last, plane])], plane, acc, 0, keep, False)

    def half_bytes(sem):
        part = half_all.at[pl.ds(0, CHIPS - 1), used]
        return pltpu.make_async_copy(part, part, sem.at[1])

    def finish_operator(step, count):
        s = WIND[0]
        high_plane(step)
        W[3] += high_x[step]
        project([(0, W[3])], 3, acc, 0, count, False)
        for part in range(PIECES[3]):
            low_plane(step, planes - 1, part)
        W[1] -= (0.5 * s) * low_x[step, 1]
        project([(0, W[1])], 1, acc, 0, count, False)
        W[0] += (1.0 + 2.0 * s) * low_x[step, 1]
        for part in range(PIECES[2]):
            where = piece(planes - 2, part)
            low_plane(step, planes - 2, part)
            W[0, where] -= (0.5 * s) * low_x[step, 0, where]
            project([(0, W[0, where])], 0, acc, 0, count, False, where)
        send_row(step, packed(acc, 0, 2 * ROWS))

    finish_operator(0, keep)

    half_bytes(gram_recv).wait()
    swap_buf[0] = jnp.sum(half_all[:, 0:5], axis=0) * inv_cells
    swap = pltpu.make_async_remote_copy(
        swap_buf.at[0],
        swap_buf.at[1],
        gram_send.at[2],
        gram_recv.at[2],
        device_id=partner,
        device_id_type=MESH,
    )
    swap.start()
    swap.wait_recv()
    even = jnp.where(core == 0, swap_buf[0], swap_buf[1])
    odd = jnp.where(core == 0, swap_buf[1], swap_buf[0])
    dense = jnp.concatenate([even[0:4], odd[0:4]], axis=0)
    parts = [dense] + [pltpu.roll(dense, 128 - block * q, 1) for q in range(1, 4)]
    square = jnp.concatenate(parts, axis=0)
    square = jnp.where(
        lax.broadcasted_iota(jnp.int32, (block, 128), 1) < block, square, 0.0
    )
    gram = jnp.concatenate([square, jnp.zeros((8, 128), f32)], axis=0)
    extra = even[4:5]
    values = [extra] + [pltpu.roll(extra, 128 - keep * q, 1) for q in range(1, 3)]
    for q in range(3):
        gram = jnp.where(row_id == block + q, values[q], gram)
    for q in range(3):
        gram = jnp.where(lane_id == block + q, as_column(values[q]), gram)
    eye = jnp.where(row_id == lane_id, 2.0, 0.0)
    lower = jnp.logical_and(row_id < last, lane_id < last)
    matrix = jnp.where(lower, eye - gram, 0.0)

    scale_row = jnp.ones((1, 128), f32)
    scale_column = jnp.ones((ROWS, 1), f32)
    results = jnp.zeros((8, 128), f32)
    row_8 = lax.broadcasted_iota(jnp.int32, (8, 128), 0)
    lane_8 = lax.broadcasted_iota(jnp.int32, (8, 128), 1)
    inverse = None
    for step in range(STEPS):
        count = keep + step
        if step > 0:
            local_part(step)
            project(
                [(0, W[2]), (ROWS, V[last + step, 2])], 2, acc, 0, count, True
            )
            for plane in (3, 1, 0):
                project([(ROWS, V[last + step, plane])], plane, acc, 0, count, False)
            if step > 1:
                for plane in range(planes):
                    out[step - 2, plane] = V[last + step - 1, plane] * inverse
            finish_operator(step, count)
        sums = get_row(step)
        if step > 0:
            square = jnp.sum(
                jnp.where(lane_row == ROWS + count - 1, sums, 0.0),
                axis=1,
                keepdims=True,
            )
            norm = jnp.sqrt(square + EPSILON)
            inverse = 1.0 / norm
            scale_row = jnp.where(lane_row == count - 1, inverse, scale_row)
            scale_column = jnp.where(row_column == count - 1, inverse, scale_column)
            results = jnp.where(
                jnp.logical_and(row_8 == step - 1, lane_8 == count - 1), norm, results
            )
            factor = scale_row * inverse
        else:
            factor = scale_row
        valid = lane_row < count
        first = jnp.where(valid, sums * factor, 0.0)
        cross = jnp.where(valid, pltpu.roll(sums, 128 - ROWS, 1) * factor, 0.0)
        cross_column = as_column(cross)
        matrix = jnp.where(row_id == count - 1, eye - cross, matrix)
        matrix = jnp.where(lane_id == count - 1, eye - cross_column, matrix)
        weights = jnp.sum(matrix * first, axis=1, keepdims=True)
        weights = jnp.where(row_column < count, weights, 0.0)
        hb[...] = jnp.broadcast_to(weights * scale_column, hb.shape)

        def combine(plane, where):
            start = W[plane, where]
            if step > 0:
                start = start * inverse

            def minus(i, total):
                return total - hb[pl.ds(i, 1), :] * V[i, plane, where]

            def four(t, total):
                for q in range(4):
                    total = minus(4 * t + q, total)
                return total

            total = lax.fori_loop(0, count // 4, four, start)
            for i in range(4 * (count // 4), count):
                total = minus(i, total)
            V[count, plane, where] = total

        more = step + 1 < STEPS
        for plane in order:
            if more and plane >= planes - 2:
                for part in range(PIECES[plane]):
                    combine(plane, piece(plane, part))
                    send_piece(step + 1, plane, part)
            else:
                combine(plane, slice(None))
            if more:
                send_rest(step + 1, plane)
        results = jnp.where(row_8 == step, as_row(weights, ROWS), results)

    total = jnp.zeros((8, 128), f32)
    for plane in range(planes):
        v = V[keep + STEPS - 1, plane]
        total = total + folded(v * v)
    square = jnp.sum(jnp.sum(total, axis=0, keepdims=True), axis=1, keepdims=True)
    send_row(STEPS, jnp.broadcast_to(square, (1, 128)))
    for plane in range(planes):
        out[STEPS - 2, plane] = V[keep + STEPS - 2, plane] * inverse
    sums = get_row(STEPS)
    norm = jnp.sqrt(sums[:, 0:1] + EPSILON)
    inverse = 1.0 / norm
    results = jnp.where(
        jnp.logical_and(row_8 == STEPS - 1, lane_8 == keep + STEPS - 1), norm, results
    )
    hess[...] = results[0:STEPS, 0:ROWS]
    for plane in range(planes):
        out[STEPS - 1, plane] = V[keep + STEPS - 1, plane] * inverse

    for step in range(STEPS):

        @pl.when(chip < CHIPS - 1)
        def _():
            for plane in (planes - 2, planes - 1):
                for part in range(PIECES[plane]):
                    to_next(step, plane, part).wait_send()

        @pl.when(chip > 0)
        def _():
            to_previous(step).wait_send()

        for plane in range(planes):
            to_side(step, plane).wait_send()
    for n in range(STEPS + 1):
        row_bytes(n, row_send).wait()
    to_pair.wait_send()
    half_bytes(gram_send).wait()
    swap.wait_send()


def put_out(vectors, columns, vectors_out, columns_out, sem):
    copies = [
        pltpu.make_async_copy(vectors, vectors_out, sem.at[0]),
        pltpu.make_async_copy(columns, columns_out, sem.at[1]),
    ]
    for copy in copies:
        copy.start()
    for copy in copies:
        copy.wait()


def body(basis_vectors, reaction):
    keep, planes, rows, cols = basis_vectors.shape
    f32 = jnp.float32
    field = (planes, rows, cols)
    dma = pltpu.SemaphoreType.DMA
    vmem = pltpu.VMEM
    reaction = pltpu.with_memory_space_constraint(reaction, pltpu.HBM)
    vectors, columns = pl.pallas_call(
        functools.partial(kernel, keep, planes, rows, cols),
        out_shape=(
            jax.ShapeDtypeStruct((STEPS, *field), f32),
            jax.ShapeDtypeStruct((STEPS, keep + STEPS), f32),
        ),
        in_specs=[pl.BlockSpec(memory_space=pltpu.HBM)] * 2,
        out_specs=(
            pl.BlockSpec(memory_space=pltpu.VMEM),
            pl.BlockSpec(memory_space=pltpu.VMEM),
        ),
        scratch_shapes=[
            vmem((keep + STEPS, *field), f32),
            vmem(field, f32),
            vmem(field, f32),
            vmem((STEPS, 2, rows, cols), f32),
            vmem((STEPS, rows, cols), f32),
            vmem((STEPS, planes, 8, cols), f32),
            vmem((2 * ROWS, 8, 128), f32),
            vmem((3 * ROWS, 8, 128), f32),
            vmem((8 * keep, 256), f32),
            vmem((8 * keep, 256), f32),
            vmem((8 * keep - 256, 256), f32),
            vmem((256, 128), f32),
            vmem((ROWS, cols), f32),
            vmem((STEPS + 1, 1, 128), f32),
            vmem((STEPS + 1, DEVICES, 1, 128), f32),
            vmem((16, 128), f32),
            vmem((8, 128), f32),
            vmem((8, 128), f32),
            vmem((CHIPS, 8, 128), f32),
            vmem((2, 5, 128), f32),
            dma((9,)),
            dma((STEPS, 2, 4)),
            dma((STEPS,)),
            dma((STEPS, 2, 4)),
            dma((STEPS,)),
            dma((STEPS, planes)),
            dma((STEPS, planes)),
            dma((STEPS + 1,)),
            dma((STEPS + 1,)),
            dma((3,)),
            dma((3,)),
        ],
        compiler_params=pltpu.CompilerParams(
            collective_id=0,
            has_side_effects=True,
            vmem_limit_bytes=48 * 1024 * 1024,
        ),
    )(basis_vectors, reaction)
    shapes = (vectors, columns)
    new_vectors, rows_out = pl.pallas_call(
        put_out,
        out_shape=tuple(jax.ShapeDtypeStruct(a.shape, f32) for a in shapes),
        in_specs=[pl.BlockSpec(memory_space=pltpu.VMEM)] * 2,
        out_specs=(pl.BlockSpec(memory_space=pl.ANY),) * 2,
        scratch_shapes=[dma((2,))],
        compiler_params=pltpu.CompilerParams(vmem_limit_bytes=4 * 1024 * 1024),
    )(vectors, columns)
    return new_vectors, rows_out.T


def solution(mesh):
    return jax.shard_map(
        body,
        mesh=mesh,
        in_specs=(P(None, "gx", "gy", None), P("gx", "gy", None)),
        out_specs=(P(None, "gx", "gy", None), P()),
        check_vma=False,
    )
```

```python
import functools

import jax
import jax.numpy as jnp
from jax import lax
from jax.experimental import pallas as pl
from jax.experimental.pallas import tpu as pltpu
from jax.sharding import PartitionSpec as P

MESH = pl.DeviceIdType.MESH
STEPS = 4
WIND = (0.9, 0.6, 0.4)
EPSILON = 1e-06
SIDE = 4
CHIPS = 64
DEVICES = 128
ROWS = 40
PIECES = {2: 4, 3: 4}


def hops(delta):
    return sum(min(d, SIDE - d) for d in delta[:3])


def partners(with_core):
    places = [
        (z, y, x, c)
        for z in range(SIDE)
        for y in range(SIDE)
        for x in range(SIDE)
        for c in range(2 if with_core else 1)
    ]
    return sorted(
        [p for p in places if any(p)], key=lambda p: (-2 * hops(p) - p[3], p[0], p[1], p[2])
    )


def kernel(
    keep,
    planes,
    rows,
    cols,
    basis,
    react,
    out,
    hess,
    V,
    W,
    RC,
    low_x,
    high_x,
    side_y,
    acc,
    acc_kept,
    gram_hh,
    gram_hl,
    gram_lh,
    gram_ll,
    hb,
    row_src,
    row_all,
    pair_src,
    pair_got,
    half_src,
    half_all,
    swap_buf,
    load_sem,
    next_send,
    x_send,
    low_recv,
    high_recv,
    y_send,
    y_recv,
    row_send,
    row_recv,
    gram_send,
    gram_recv,
):
    f32 = jnp.float32
    core = lax.axis_index("gy")
    chip = lax.axis_index("gx")
    me = core * CHIPS + chip
    cz, cy, cx = lax.div(chip, 16), lax.rem(lax.div(chip, 4), 4), lax.rem(chip, 4)
    zs = [lax.rem(cz + d, SIDE) * 16 for d in range(SIDE)]
    ys = [lax.rem(cy + d, SIDE) * 4 for d in range(SIDE)]
    xs = [lax.rem(cx + d, SIDE) for d in range(SIDE)]
    cores = [core, 1 - core]
    inv_cells = 1.0 / float(DEVICES * planes * rows * cols)

    def device(place):
        z, y, x, c = place
        return {"gy": cores[c], "gx": zs[z] + ys[y] + xs[x]}

    last = keep - 1
    loads = [
        pltpu.make_async_copy(basis.at[last], V.at[last], load_sem.at[0]),
        pltpu.make_async_copy(react, RC, load_sem.at[1]),
    ]
    for n, start in enumerate(range(0, last, 7)):
        part = pl.ds(start, min(7, last - start))
        loads.append(
            pltpu.make_async_copy(basis.at[part], V.at[part], load_sem.at[2 + n])
        )
    for copy in loads:
        copy.start()

    barrier = pltpu.get_barrier_semaphore()
    for place in partners(True):
        pl.semaphore_signal(
            barrier, inc=1, device_id=device(place), device_id_type=MESH
        )

    acc[...] = jnp.zeros(acc.shape, f32)
    acc_kept[...] = jnp.zeros(acc_kept.shape, f32)
    gram_hh[...] = jnp.zeros(gram_hh.shape, f32)
    gram_hl[...] = jnp.zeros(gram_hl.shape, f32)
    gram_lh[...] = jnp.zeros(gram_lh.shape, f32)
    gram_ll[...] = jnp.zeros(gram_ll.shape, f32)

    @pl.when(chip == 0)
    def _():
        low_x[...] = jnp.zeros(low_x.shape, f32)

    @pl.when(chip == CHIPS - 1)
    def _():
        high_x[...] = jnp.zeros(high_x.shape, f32)

    def piece(plane, part):
        size = rows // PIECES[plane]
        return pl.ds(part * size, size)

    def to_next(step, plane, part):
        place, where = plane - (planes - 2), piece(plane, part)
        return pltpu.make_async_remote_copy(
            V.at[last + step, plane, where],
            low_x.at[step, place, where],
            next_send.at[step, place, part],
            low_recv.at[step, place, part],
            device_id={"gy": core, "gx": lax.rem(chip + 1, CHIPS)},
            device_id_type=MESH,
        )

    def to_previous(step):
        return pltpu.make_async_remote_copy(
            V.at[last + step, 0],
            high_x.at[step],
            x_send.at[step],
            high_recv.at[step],
            device_id={"gy": core, "gx": lax.rem(chip + CHIPS - 1, CHIPS)},
            device_id_type=MESH,
        )

    edge = pl.ds(pl.multiple_of((1 - core) * (rows - 8), 8), 8)

    def to_side(step, plane):
        return pltpu.make_async_remote_copy(
            V.at[last + step, plane, edge],
            side_y.at[step, plane],
            y_send.at[step, plane],
            y_recv.at[step, plane],
            device_id={"gy": 1 - core, "gx": chip},
            device_id_type=MESH,
        )

    def send_piece(step, plane, part):
        @pl.when(chip < CHIPS - 1)
        def _():
            to_next(step, plane, part).start()

    def send_rest(step, plane):
        if plane == 0:

            @pl.when(chip > 0)
            def _():
                to_previous(step).start()

        to_side(step, plane).start()

    def send_plane(step, plane):
        if plane >= planes - 2:
            for part in range(PIECES[plane]):
                send_piece(step, plane, part)
        send_rest(step, plane)

    order = (3, 0, 2, 1)

    lanes = lax.broadcasted_iota(jnp.int32, (rows, cols), 1)

    def local_part(step):
        centre = 6.0 + 1.5 * sum(WIND)
        index = last + step
        for plane in range(planes):
            to_side(step, plane).wait_recv()
        for plane in range(planes):
            v = V[index, plane]
            side = side_y[step, plane]
            below = jnp.where(core == 1, side, 0.0)
            above = jnp.where(core == 0, side, 0.0)
            tall = jnp.concatenate([below, v, above], axis=0)
            total = -(RC[plane] + centre) * v
            s = WIND[1]
            total += tall[9 : rows + 9]
            total += (1.0 + 2.0 * s) * tall[7 : rows + 7] - (0.5 * s) * tall[6 : rows + 6]
            s = WIND[2]
            total += jnp.where(lanes < cols - 1, pltpu.roll(v, cols - 1, 1), 0.0)
            total += (1.0 + 2.0 * s) * jnp.where(lanes >= 1, pltpu.roll(v, 1, 1), 0.0)
            total -= (0.5 * s) * jnp.where(lanes >= 2, pltpu.roll(v, 2, 1), 0.0)
            s = WIND[0]
            if plane + 1 < planes:
                total += V[index, plane + 1]
            if plane >= 1:
                total += (1.0 + 2.0 * s) * V[index, plane - 1]
            if plane >= 2:
                total -= (0.5 * s) * V[index, plane - 2]
            W[plane] = total

    def low_plane(step, plane, part):
        @pl.when(chip > 0)
        def _():
            to_next(step, plane, part).wait_recv()

    def high_plane(step):
        @pl.when(chip < CHIPS - 1)
        def _():
            to_previous(step).wait_recv()

    def folded(product):
        half = product[:, : cols // 2] + product[:, cols // 2 :]
        parts = [half[8 * t : 8 * t + 8] for t in range(product.shape[0] // 8)]
        while len(parts) > 1:
            parts = [a + b for a, b in zip(parts[::2], parts[1::2])]
        return parts[0]

    def project(operands, plane, target, first, count, fresh, where=slice(None)):
        def one(i):
            v = V[i, plane, where]
            for offset, w in operands:
                part = folded(v * w)
                target[offset + i] = part if fresh else target[offset + i] + part

        fours = (count - first) // 4

        def four(t, carry):
            for q in range(4):
                one(first + 4 * t + q)
            return carry

        lax.fori_loop(0, fours, four, 0)
        for i in range(first + 4 * fours, count):
            one(i)

    def diagonal(shape):
        return lax.broadcasted_iota(jnp.int32, shape, 0) == lax.broadcasted_iota(
            jnp.int32, shape, 1
        )

    def as_row(column, count):
        return jnp.sum(
            jnp.where(diagonal((count, 128)), column, 0.0), axis=0, keepdims=True
        )

    def as_column(row):
        return jnp.sum(
            jnp.where(diagonal((ROWS, 128)), row, 0.0), axis=1, keepdims=True
        )

    def packed(ref, start, count):
        flat = jnp.sum(ref[start : start + count], axis=1)
        return as_row(jnp.sum(flat, axis=1, keepdims=True), count)

    def send_row(n, row):
        row_src[n] = row
        row_all[n, me] = row
        for place in partners(True):
            pltpu.make_async_remote_copy(
                row_src.at[n],
                row_all.at[n, me],
                row_send.at[n],
                row_recv.at[n],
                device_id=device(place),
                device_id_type=MESH,
            ).start()

    def row_bytes(n, sem):
        part = row_all.at[n, pl.ds(0, DEVICES - 1)]
        return pltpu.make_async_copy(part, part, sem.at[n])

    def get_row(n):
        row_bytes(n, row_recv).wait()
        return jnp.sum(row_all[n], axis=0) * inv_cells

    row_id = lax.broadcasted_iota(jnp.int32, (ROWS, 128), 0)
    lane_id = lax.broadcasted_iota(jnp.int32, (ROWS, 128), 1)
    lane_row = lax.broadcasted_iota(jnp.int32, (1, 128), 1)
    row_column = lax.broadcasted_iota(jnp.int32, (ROWS, 1), 0)

    loads[0].wait()
    for copy in loads[2:]:
        copy.wait()
    block = 32
    size = block * 8
    tall = keep * 8

    def gram_tile(tile, carry):
        start = pl.multiple_of(tile * 8, 8)
        v = jnp.concatenate(
            [
                V[0:keep, plane, pl.ds(start, 8), :].reshape(tall, cols)
                for plane in range(planes)
            ],
            axis=1,
        )
        high = v.astype(jnp.bfloat16)
        rest = v - high.astype(f32)
        low = rest.astype(jnp.bfloat16)

        def product(a, b):
            return lax.dot_general(
                a, b, (((1,), (1,)), ((), ())), preferred_element_type=f32
            )

        gram_hh[...] += product(high, high[0:size])
        gram_hl[...] += product(high, low[0:size])
        gram_lh[...] += product(low[size:], high[0:size])
        square = rest[0:size] * rest[0:size]
        parts = [square[:, 128 * n : 128 * n + 128] for n in range(planes * cols // 128)]
        while len(parts) > 1:
            parts = [a + b for a, b in zip(parts[::2], parts[1::2])]
        gram_ll[...] += parts[0]
        return carry

    early = 2
    lax.fori_loop(0, early, gram_tile, 0)
    pl.semaphore_wait(barrier, DEVICES - 1)
    for plane in order:
        send_plane(0, plane)
    lax.fori_loop(early, rows // 8, gram_tile, 0)
    for plane in range(planes):
        project(
            [(ROWS * q, V[block + q, plane]) for q in range(3)],
            plane,
            acc_kept,
            block,
            last,
            plane == 0,
        )

    pick = (
        lax.div(lax.broadcasted_iota(jnp.int32, (size, 128), 0), 8)
        == lax.broadcasted_iota(jnp.int32, (size, 128), 1)
    ).astype(f32)

    def blocks(matrix):
        count = matrix.shape[0]
        same = lax.rem(
            lax.broadcasted_iota(jnp.int32, (count, size), 0), 8
        ) == lax.rem(lax.broadcasted_iota(jnp.int32, (count, size), 1), 8)
        kept = jnp.where(same, matrix, 0.0).reshape(count // 8, 8, size)
        return jnp.sum(kept, axis=1)

    stacked = jnp.concatenate(
        [
            blocks(0.5 * gram_hh[0:size] + gram_hl[0:size]),
            blocks(gram_hh[size:] + gram_hl[size:] + gram_lh[...]),
        ],
        axis=0,
    )
    inner = jnp.dot(
        stacked, pick, precision=lax.Precision.HIGHEST, preferred_element_type=f32
    )
    ll = jnp.sum(
        jnp.sum(gram_ll[...].reshape(block, 8, 128), axis=1), axis=1, keepdims=True
    )
    turned = jnp.concatenate([inner[0:block], jnp.zeros((96, 128), f32)], axis=0).T
    square = inner[0:block] + turned[0:block]
    square = square + jnp.where(diagonal((block, 128)), ll, 0.0)
    dense = square[0:8]
    for q in range(1, 4):
        dense = dense + pltpu.roll(square[8 * q : 8 * q + 8], block * q, 1)
    extra = jnp.zeros((1, 128), f32)
    for q in range(3):
        exact = packed(acc_kept, ROWS * q, ROWS)
        values = inner[block + q : block + q + 1]
        values = jnp.where(lane_row < block, values, exact)
        values = jnp.where(lane_row < keep, values, 0.0)
        extra = extra + (pltpu.roll(values, keep * q, 1) if q else values)
    pair_src[0:4] = dense[0:4]
    pair_src[4:5] = extra
    pair_src[5:8] = jnp.zeros((3, 128), f32)
    pair_src[8:12] = dense[4:8]
    pair_src[12:16] = jnp.zeros((4, 128), f32)
    theirs = pl.ds(pl.multiple_of((1 - core) * 8, 8), 8)
    partner = {"gy": 1 - core, "gx": chip}
    to_pair = pltpu.make_async_remote_copy(
        pair_src.at[theirs],
        pair_got,
        gram_send.at[0],
        gram_recv.at[0],
        device_id=partner,
        device_id_type=MESH,
    )
    to_pair.start()
    loads[1].wait()
    local_part(0)
    project([(0, W[2]), (ROWS, V[last, 2])], 2, acc, 0, keep, True)
    to_pair.wait_recv()
    mine = jnp.where(core == 0, pair_src[0:8], pair_src[8:16]) + pair_got[...]
    used = pl.ds(0, 5)
    half_src[...] = mine
    half_all[chip, 0:5] = mine[0:5]
    for place in partners(False):
        pltpu.make_async_remote_copy(
            half_src.at[used],
            half_all.at[chip, used],
            gram_send.at[1],
            gram_recv.at[1],
            device_id=device(place),
            device_id_type=MESH,
        ).start()

    for plane in (3, 1, 0):
        project([(ROWS, V[last, plane])], plane, acc, 0, keep, False)

    def half_bytes(sem):
        part = half_all.at[pl.ds(0, CHIPS - 1), used]
        return pltpu.make_async_copy(part, part, sem.at[1])

    def finish_operator(step, count):
        s = WIND[0]
        high_plane(step)
        W[3] += high_x[step]
        project([(0, W[3])], 3, acc, 0, count, False)
        for part in range(PIECES[3]):
            low_plane(step, planes - 1, part)
        W[1] -= (0.5 * s) * low_x[step, 1]
        project([(0, W[1])], 1, acc, 0, count, False)
        W[0] += (1.0 + 2.0 * s) * low_x[step, 1]
        for part in range(PIECES[2]):
            where = piece(planes - 2, part)
            low_plane(step, planes - 2, part)
            W[0, where] -= (0.5 * s) * low_x[step, 0, where]
            project([(0, W[0, where])], 0, acc, 0, count, False, where)
        send_row(step, packed(acc, 0, 2 * ROWS))

    finish_operator(0, keep)

    half_bytes(gram_recv).wait()
    swap_buf[0] = jnp.sum(half_all[:, 0:5], axis=0) * inv_cells
    swap = pltpu.make_async_remote_copy(
        swap_buf.at[0],
        swap_buf.at[1],
        gram_send.at[2],
        gram_recv.at[2],
        device_id=partner,
        device_id_type=MESH,
    )
    swap.start()
    swap.wait_recv()
    even = jnp.where(core == 0, swap_buf[0], swap_buf[1])
    odd = jnp.where(core == 0, swap_buf[1], swap_buf[0])
    dense = jnp.concatenate([even[0:4], odd[0:4]], axis=0)
    parts = [dense] + [pltpu.roll(dense, 128 - block * q, 1) for q in range(1, 4)]
    square = jnp.concatenate(parts, axis=0)
    square = jnp.where(
        lax.broadcasted_iota(jnp.int32, (block, 128), 1) < block, square, 0.0
    )
    gram = jnp.concatenate([square, jnp.zeros((8, 128), f32)], axis=0)
    extra = even[4:5]
    values = [extra] + [pltpu.roll(extra, 128 - keep * q, 1) for q in range(1, 3)]
    for q in range(3):
        gram = jnp.where(row_id == block + q, values[q], gram)
    for q in range(3):
        gram = jnp.where(lane_id == block + q, as_column(values[q]), gram)
    eye = jnp.where(row_id == lane_id, 2.0, 0.0)
    lower = jnp.logical_and(row_id < last, lane_id < last)
    matrix = jnp.where(lower, eye - gram, 0.0)

    scale_row = jnp.ones((1, 128), f32)
    scale_column = jnp.ones((ROWS, 1), f32)
    results = jnp.zeros((8, 128), f32)
    row_8 = lax.broadcasted_iota(jnp.int32, (8, 128), 0)
    lane_8 = lax.broadcasted_iota(jnp.int32, (8, 128), 1)
    inverse = None
    for step in range(STEPS):
        count = keep + step
        if step > 0:
            local_part(step)
            project(
                [(0, W[2]), (ROWS, V[last + step, 2])], 2, acc, 0, count, True
            )
            for plane in (3, 1, 0):
                project([(ROWS, V[last + step, plane])], plane, acc, 0, count, False)
            if step > 1:
                for plane in range(planes):
                    out[step - 2, plane] = V[last + step - 1, plane] * inverse
            finish_operator(step, count)
        sums = get_row(step)
        if step > 0:
            square = jnp.sum(
                jnp.where(lane_row == ROWS + count - 1, sums, 0.0),
                axis=1,
                keepdims=True,
            )
            norm = jnp.sqrt(square + EPSILON)
            inverse = 1.0 / norm
            scale_row = jnp.where(lane_row == count - 1, inverse, scale_row)
            scale_column = jnp.where(row_column == count - 1, inverse, scale_column)
            results = jnp.where(
                jnp.logical_and(row_8 == step - 1, lane_8 == count - 1), norm, results
            )
            factor = scale_row * inverse
        else:
            factor = scale_row
        valid = lane_row < count
        first = jnp.where(valid, sums * factor, 0.0)
        cross = jnp.where(valid, pltpu.roll(sums, 128 - ROWS, 1) * factor, 0.0)
        cross_column = as_column(cross)
        matrix = jnp.where(row_id == count - 1, eye - cross, matrix)
        matrix = jnp.where(lane_id == count - 1, eye - cross_column, matrix)
        weights = jnp.sum(matrix * first, axis=1, keepdims=True)
        weights = jnp.where(row_column < count, weights, 0.0)
        hb[...] = jnp.broadcast_to(weights * scale_column, hb.shape)

        def combine(plane, where):
            start = W[plane, where]
            if step > 0:
                start = start * inverse

            def minus(i, total):
                return total - hb[pl.ds(i, 1), :] * V[i, plane, where]

            def four(t, total):
                for q in range(4):
                    total = minus(4 * t + q, total)
                return total

            total = lax.fori_loop(0, count // 4, four, start)
            for i in range(4 * (count // 4), count):
                total = minus(i, total)
            V[count, plane, where] = total

        more = step + 1 < STEPS
        for plane in order:
            if more and plane >= planes - 2:
                for part in range(PIECES[plane]):
                    combine(plane, piece(plane, part))
                    send_piece(step + 1, plane, part)
            else:
                combine(plane, slice(None))
            if more:
                send_rest(step + 1, plane)
        results = jnp.where(row_8 == step, as_row(weights, ROWS), results)

    total = jnp.zeros((8, 128), f32)
    for plane in range(planes):
        v = V[keep + STEPS - 1, plane]
        total = total + folded(v * v)
    square = jnp.sum(jnp.sum(total, axis=0, keepdims=True), axis=1, keepdims=True)
    send_row(STEPS, jnp.broadcast_to(square, (1, 128)))
    for plane in range(planes):
        out[STEPS - 2, plane] = V[keep + STEPS - 2, plane] * inverse
    sums = get_row(STEPS)
    norm = jnp.sqrt(sums[:, 0:1] + EPSILON)
    inverse = 1.0 / norm
    results = jnp.where(
        jnp.logical_and(row_8 == STEPS - 1, lane_8 == keep + STEPS - 1), norm, results
    )
    hess[...] = results[0:STEPS, 0:ROWS]
    for plane in range(planes):
        out[STEPS - 1, plane] = V[keep + STEPS - 1, plane] * inverse

    for step in range(STEPS):

        @pl.when(chip < CHIPS - 1)
        def _():
            for plane in (planes - 2, planes - 1):
                for part in range(PIECES[plane]):
                    to_next(step, plane, part).wait_send()

        @pl.when(chip > 0)
        def _():
            to_previous(step).wait_send()

        for plane in range(planes):
            to_side(step, plane).wait_send()
    for n in range(STEPS + 1):
        row_bytes(n, row_send).wait()
    to_pair.wait_send()
    half_bytes(gram_send).wait()
    swap.wait_send()


def put_out(vectors, columns, vectors_out, columns_out, sem):
    copies = [
        pltpu.make_async_copy(vectors, vectors_out, sem.at[0]),
        pltpu.make_async_copy(columns, columns_out, sem.at[1]),
    ]
    for copy in copies:
        copy.start()
    for copy in copies:
        copy.wait()


def body(basis_vectors, reaction):
    keep, planes, rows, cols = basis_vectors.shape
    f32 = jnp.float32
    field = (planes, rows, cols)
    dma = pltpu.SemaphoreType.DMA
    vmem = pltpu.VMEM
    reaction = pltpu.with_memory_space_constraint(reaction, pltpu.HBM)
    vectors, columns = pl.pallas_call(
        functools.partial(kernel, keep, planes, rows, cols),
        out_shape=(
            jax.ShapeDtypeStruct((STEPS, *field), f32),
            jax.ShapeDtypeStruct((STEPS, keep + STEPS), f32),
        ),
        in_specs=[pl.BlockSpec(memory_space=pltpu.HBM)] * 2,
        out_specs=(
            pl.BlockSpec(memory_space=pltpu.VMEM),
            pl.BlockSpec(memory_space=pltpu.VMEM),
        ),
        scratch_shapes=[
            vmem((keep + STEPS, *field), f32),
            vmem(field, f32),
            vmem(field, f32),
            vmem((STEPS, 2, rows, cols), f32),
            vmem((STEPS, rows, cols), f32),
            vmem((STEPS, planes, 8, cols), f32),
            vmem((2 * ROWS, 8, 128), f32),
            vmem((3 * ROWS, 8, 128), f32),
            vmem((8 * keep, 256), f32),
            vmem((8 * keep, 256), f32),
            vmem((8 * keep - 256, 256), f32),
            vmem((256, 128), f32),
            vmem((ROWS, cols), f32),
            vmem((STEPS + 1, 1, 128), f32),
            vmem((STEPS + 1, DEVICES, 1, 128), f32),
            vmem((16, 128), f32),
            vmem((8, 128), f32),
            vmem((8, 128), f32),
            vmem((CHIPS, 8, 128), f32),
            vmem((2, 5, 128), f32),
            dma((9,)),
            dma((STEPS, 2, 4)),
            dma((STEPS,)),
            dma((STEPS, 2, 4)),
            dma((STEPS,)),
            dma((STEPS, planes)),
            dma((STEPS, planes)),
            dma((STEPS + 1,)),
            dma((STEPS + 1,)),
            dma((3,)),
            dma((3,)),
        ],
        compiler_params=pltpu.CompilerParams(
            collective_id=0,
            has_side_effects=True,
            vmem_limit_bytes=48 * 1024 * 1024,
        ),
    )(basis_vectors, reaction)
    shapes = (vectors, columns)
    new_vectors, rows_out = pl.pallas_call(
        put_out,
        out_shape=tuple(jax.ShapeDtypeStruct(a.shape, f32) for a in shapes),
        in_specs=[pl.BlockSpec(memory_space=pltpu.VMEM)] * 2,
        out_specs=(pl.BlockSpec(memory_space=pl.ANY),) * 2,
        scratch_shapes=[dma((2,))],
        compiler_params=pltpu.CompilerParams(vmem_limit_bytes=4 * 1024 * 1024),
    )(vectors, columns)
    return new_vectors, rows_out.T


def solution(mesh):
    return jax.shard_map(
        body,
        mesh=mesh,
        in_specs=(P(None, "gx", "gy", None), P("gx", "gy", None)),
        out_specs=(P(None, "gx", "gy", None), P()),
        check_vma=False,
    )
```

```python
import functools

import jax
import jax.numpy as jnp
from jax import lax
from jax.experimental import pallas as pl
from jax.experimental.pallas import tpu as pltpu
from jax.sharding import PartitionSpec as P

MESH = pl.DeviceIdType.MESH
STEPS = 4
WIND = (0.9, 0.6, 0.4)
EPSILON = 1e-06
SIDE = 4
CHIPS = 64
DEVICES = 128
ROWS = 40
PIECES = {2: 4, 3: 4}


def hops(delta):
    return sum(min(d, SIDE - d) for d in delta[:3])


def partners(with_core):
    places = [
        (z, y, x, c)
        for z in range(SIDE)
        for y in range(SIDE)
        for x in range(SIDE)
        for c in range(2 if with_core else 1)
    ]
    return sorted(
        [p for p in places if any(p)], key=lambda p: (-2 * hops(p) - p[3], p[0], p[1], p[2])
    )


def kernel(
    keep,
    planes,
    rows,
    cols,
    basis,
    react,
    out,
    hess,
    V,
    W,
    RC,
    low_x,
    high_x,
    side_y,
    acc,
    acc_kept,
    gram_hh,
    gram_hl,
    gram_lh,
    gram_ll,
    hb,
    row_src,
    row_all,
    pair_src,
    pair_got,
    half_src,
    half_all,
    swap_buf,
    load_sem,
    next_send,
    x_send,
    low_recv,
    high_recv,
    y_send,
    y_recv,
    row_send,
    row_recv,
    gram_send,
    gram_recv,
):
    f32 = jnp.float32
    core = lax.axis_index("gy")
    chip = lax.axis_index("gx")
    me = core * CHIPS + chip
    cz, cy, cx = lax.div(chip, 16), lax.rem(lax.div(chip, 4), 4), lax.rem(chip, 4)
    zs = [lax.rem(cz + d, SIDE) * 16 for d in range(SIDE)]
    ys = [lax.rem(cy + d, SIDE) * 4 for d in range(SIDE)]
    xs = [lax.rem(cx + d, SIDE) for d in range(SIDE)]
    cores = [core, 1 - core]
    inv_cells = 1.0 / float(DEVICES * planes * rows * cols)

    def device(place):
        z, y, x, c = place
        return {"gy": cores[c], "gx": zs[z] + ys[y] + xs[x]}

    last = keep - 1
    loads = [
        pltpu.make_async_copy(basis.at[last], V.at[last], load_sem.at[0]),
        pltpu.make_async_copy(react, RC, load_sem.at[1]),
    ]
    for n, start in enumerate(range(0, last, 7)):
        part = pl.ds(start, min(7, last - start))
        loads.append(
            pltpu.make_async_copy(basis.at[part], V.at[part], load_sem.at[2 + n])
        )
    for copy in loads:
        copy.start()

    barrier = pltpu.get_barrier_semaphore()
    for place in partners(True):
        pl.semaphore_signal(
            barrier, inc=1, device_id=device(place), device_id_type=MESH
        )

    acc[...] = jnp.zeros(acc.shape, f32)
    acc_kept[...] = jnp.zeros(acc_kept.shape, f32)
    gram_hh[...] = jnp.zeros(gram_hh.shape, f32)
    gram_hl[...] = jnp.zeros(gram_hl.shape, f32)
    gram_lh[...] = jnp.zeros(gram_lh.shape, f32)
    gram_ll[...] = jnp.zeros(gram_ll.shape, f32)

    @pl.when(chip == 0)
    def _():
        low_x[...] = jnp.zeros(low_x.shape, f32)

    @pl.when(chip == CHIPS - 1)
    def _():
        high_x[...] = jnp.zeros(high_x.shape, f32)

    def piece(plane, part):
        size = rows // PIECES[plane]
        return pl.ds(part * size, size)

    def to_next(step, plane, part):
        place, where = plane - (planes - 2), piece(plane, part)
        return pltpu.make_async_remote_copy(
            V.at[last + step, plane, where],
            low_x.at[step, place, where],
            next_send.at[step, place, part],
            low_recv.at[step, place, part],
            device_id={"gy": core, "gx": lax.rem(chip + 1, CHIPS)},
            device_id_type=MESH,
        )

    def to_previous(step):
        return pltpu.make_async_remote_copy(
            V.at[last + step, 0],
            high_x.at[step],
            x_send.at[step],
            high_recv.at[step],
            device_id={"gy": core, "gx": lax.rem(chip + CHIPS - 1, CHIPS)},
            device_id_type=MESH,
        )

    edge = pl.ds(pl.multiple_of((1 - core) * (rows - 8), 8), 8)

    def to_side(step, plane):
        return pltpu.make_async_remote_copy(
            V.at[last + step, plane, edge],
            side_y.at[step, plane],
            y_send.at[step, plane],
            y_recv.at[step, plane],
            device_id={"gy": 1 - core, "gx": chip},
            device_id_type=MESH,
        )

    def send_piece(step, plane, part):
        @pl.when(chip < CHIPS - 1)
        def _():
            to_next(step, plane, part).start()

    def send_rest(step, plane):
        if plane == 0:

            @pl.when(chip > 0)
            def _():
                to_previous(step).start()

        to_side(step, plane).start()

    def send_plane(step, plane):
        if plane >= planes - 2:
            for part in range(PIECES[plane]):
                send_piece(step, plane, part)
        send_rest(step, plane)

    order = (3, 0, 2, 1)

    lanes = lax.broadcasted_iota(jnp.int32, (rows, cols), 1)

    def local_part(step):
        centre = 6.0 + 1.5 * sum(WIND)
        index = last + step
        for plane in range(planes):
            to_side(step, plane).wait_recv()
        for plane in range(planes):
            v = V[index, plane]
            side = side_y[step, plane]
            below = jnp.where(core == 1, side, 0.0)
            above = jnp.where(core == 0, side, 0.0)
            tall = jnp.concatenate([below, v, above], axis=0)
            total = -(RC[plane] + centre) * v
            s = WIND[1]
            total += tall[9 : rows + 9]
            total += (1.0 + 2.0 * s) * tall[7 : rows + 7] - (0.5 * s) * tall[6 : rows + 6]
            s = WIND[2]
            total += jnp.where(lanes < cols - 1, pltpu.roll(v, cols - 1, 1), 0.0)
            total += (1.0 + 2.0 * s) * jnp.where(lanes >= 1, pltpu.roll(v, 1, 1), 0.0)
            total -= (0.5 * s) * jnp.where(lanes >= 2, pltpu.roll(v, 2, 1), 0.0)
            s = WIND[0]
            if plane + 1 < planes:
                total += V[index, plane + 1]
            if plane >= 1:
                total += (1.0 + 2.0 * s) * V[index, plane - 1]
            if plane >= 2:
                total -= (0.5 * s) * V[index, plane - 2]
            W[plane] = total

    def low_plane(step, plane, part):
        @pl.when(chip > 0)
        def _():
            to_next(step, plane, part).wait_recv()

    def high_plane(step):
        @pl.when(chip < CHIPS - 1)
        def _():
            to_previous(step).wait_recv()

    def folded(product):
        half = product[:, : cols // 2] + product[:, cols // 2 :]
        parts = [half[8 * t : 8 * t + 8] for t in range(product.shape[0] // 8)]
        while len(parts) > 1:
            parts = [a + b for a, b in zip(parts[::2], parts[1::2])]
        return parts[0]

    def project(operands, plane, target, first, count, fresh, where=slice(None)):
        def one(i):
            v = V[i, plane, where]
            for offset, w in operands:
                part = folded(v * w)
                target[offset + i] = part if fresh else target[offset + i] + part

        fours = (count - first) // 4

        def four(t, carry):
            for q in range(4):
                one(first + 4 * t + q)
            return carry

        lax.fori_loop(0, fours, four, 0)
        for i in range(first + 4 * fours, count):
            one(i)

    def diagonal(shape):
        return lax.broadcasted_iota(jnp.int32, shape, 0) == lax.broadcasted_iota(
            jnp.int32, shape, 1
        )

    def as_row(column, count):
        return jnp.sum(
            jnp.where(diagonal((count, 128)), column, 0.0), axis=0, keepdims=True
        )

    def as_column(row):
        return jnp.sum(
            jnp.where(diagonal((ROWS, 128)), row, 0.0), axis=1, keepdims=True
        )

    def packed(ref, start, count):
        flat = jnp.sum(ref[start : start + count], axis=1)
        return as_row(jnp.sum(flat, axis=1, keepdims=True), count)

    def send_row(n, row):
        row_src[n] = row
        row_all[n, me] = row
        for place in partners(True):
            pltpu.make_async_remote_copy(
                row_src.at[n],
                row_all.at[n, me],
                row_send.at[n],
                row_recv.at[n],
                device_id=device(place),
                device_id_type=MESH,
            ).start()

    def row_bytes(n, sem):
        part = row_all.at[n, pl.ds(0, DEVICES - 1)]
        return pltpu.make_async_copy(part, part, sem.at[n])

    def get_row(n):
        row_bytes(n, row_recv).wait()
        return jnp.sum(row_all[n], axis=0) * inv_cells

    row_id = lax.broadcasted_iota(jnp.int32, (ROWS, 128), 0)
    lane_id = lax.broadcasted_iota(jnp.int32, (ROWS, 128), 1)
    lane_row = lax.broadcasted_iota(jnp.int32, (1, 128), 1)
    row_column = lax.broadcasted_iota(jnp.int32, (ROWS, 1), 0)

    loads[0].wait()
    for copy in loads[2:]:
        copy.wait()
    block = 32
    size = block * 8
    tall = keep * 8

    def gram_tile(tile, carry):
        start = pl.multiple_of(tile * 8, 8)
        v = jnp.concatenate(
            [
                V[0:keep, plane, pl.ds(start, 8), :].reshape(tall, cols)
                for plane in range(planes)
            ],
            axis=1,
        )
        high = v.astype(jnp.bfloat16)
        rest = v - high.astype(f32)
        low = rest.astype(jnp.bfloat16)

        def product(a, b):
            return lax.dot_general(
                a, b, (((1,), (1,)), ((), ())), preferred_element_type=f32
            )

        gram_hh[...] += product(high, high[0:size])
        gram_hl[...] += product(high, low[0:size])
        gram_lh[...] += product(low[size:], high[0:size])
        square = rest[0:size] * rest[0:size]
        parts = [square[:, 128 * n : 128 * n + 128] for n in range(planes * cols // 128)]
        while len(parts) > 1:
            parts = [a + b for a, b in zip(parts[::2], parts[1::2])]
        gram_ll[...] += parts[0]
        return carry

    early = 2
    lax.fori_loop(0, early, gram_tile, 0)
    pl.semaphore_wait(barrier, DEVICES - 1)
    for plane in order:
        send_plane(0, plane)
    lax.fori_loop(early, rows // 8, gram_tile, 0)
    for plane in range(planes):
        project(
            [(ROWS * q, V[block + q, plane]) for q in range(3)],
            plane,
            acc_kept,
            block,
            last,
            plane == 0,
        )

    pick = (
        lax.div(lax.broadcasted_iota(jnp.int32, (size, 128), 0), 8)
        == lax.broadcasted_iota(jnp.int32, (size, 128), 1)
    ).astype(f32)

    def blocks(matrix):
        count = matrix.shape[0]
        same = lax.rem(
            lax.broadcasted_iota(jnp.int32, (count, size), 0), 8
        ) == lax.rem(lax.broadcasted_iota(jnp.int32, (count, size), 1), 8)
        kept = jnp.where(same, matrix, 0.0).reshape(count // 8, 8, size)
        return jnp.sum(kept, axis=1)

    stacked = jnp.concatenate(
        [
            blocks(0.5 * gram_hh[0:size] + gram_hl[0:size]),
            blocks(gram_hh[size:] + gram_hl[size:] + gram_lh[...]),
        ],
        axis=0,
    )
    inner = jnp.dot(
        stacked, pick, precision=lax.Precision.HIGHEST, preferred_element_type=f32
    )
    ll = jnp.sum(
        jnp.sum(gram_ll[...].reshape(block, 8, 128), axis=1), axis=1, keepdims=True
    )
    turned = jnp.concatenate([inner[0:block], jnp.zeros((96, 128), f32)], axis=0).T
    square = inner[0:block] + turned[0:block]
    square = square + jnp.where(diagonal((block, 128)), ll, 0.0)
    dense = square[0:8]
    for q in range(1, 4):
        dense = dense + pltpu.roll(square[8 * q : 8 * q + 8], block * q, 1)
    extra = jnp.zeros((1, 128), f32)
    for q in range(3):
        exact = packed(acc_kept, ROWS * q, ROWS)
        values = inner[block + q : block + q + 1]
        values = jnp.where(lane_row < block, values, exact)
        values = jnp.where(lane_row < keep, values, 0.0)
        extra = extra + (pltpu.roll(values, keep * q, 1) if q else values)
    pair_src[0:4] = dense[0:4]
    pair_src[4:5] = extra
    pair_src[5:8] = jnp.zeros((3, 128), f32)
    pair_src[8:12] = dense[4:8]
    pair_src[12:16] = jnp.zeros((4, 128), f32)
    theirs = pl.ds(pl.multiple_of((1 - core) * 8, 8), 8)
    partner = {"gy": 1 - core, "gx": chip}
    to_pair = pltpu.make_async_remote_copy(
        pair_src.at[theirs],
        pair_got,
        gram_send.at[0],
        gram_recv.at[0],
        device_id=partner,
        device_id_type=MESH,
    )
    to_pair.start()
    loads[1].wait()
    local_part(0)
    project([(0, W[2]), (ROWS, V[last, 2])], 2, acc, 0, keep, True)
    to_pair.wait_recv()
    mine = jnp.where(core == 0, pair_src[0:8], pair_src[8:16]) + pair_got[...]
    used = pl.ds(0, 5)
    half_src[...] = mine
    half_all[chip, 0:5] = mine[0:5]
    for place in partners(False):
        pltpu.make_async_remote_copy(
            half_src.at[used],
            half_all.at[chip, used],
            gram_send.at[1],
            gram_recv.at[1],
            device_id=device(place),
            device_id_type=MESH,
        ).start()

    for plane in (3, 1, 0):
        project([(ROWS, V[last, plane])], plane, acc, 0, keep, False)

    def half_bytes(sem):
        part = half_all.at[pl.ds(0, CHIPS - 1), used]
        return pltpu.make_async_copy(part, part, sem.at[1])

    def finish_operator(step, count):
        s = WIND[0]
        high_plane(step)
        W[3] += high_x[step]
        project([(0, W[3])], 3, acc, 0, count, False)
        for part in range(PIECES[3]):
            low_plane(step, planes - 1, part)
        W[1] -= (0.5 * s) * low_x[step, 1]
        project([(0, W[1])], 1, acc, 0, count, False)
        W[0] += (1.0 + 2.0 * s) * low_x[step, 1]
        for part in range(PIECES[2]):
            where = piece(planes - 2, part)
            low_plane(step, planes - 2, part)
            W[0, where] -= (0.5 * s) * low_x[step, 0, where]
            project([(0, W[0, where])], 0, acc, 0, count, False, where)
        send_row(step, packed(acc, 0, 2 * ROWS))

    finish_operator(0, keep)

    half_bytes(gram_recv).wait()
    swap_buf[0] = jnp.sum(half_all[:, 0:5], axis=0) * inv_cells
    swap = pltpu.make_async_remote_copy(
        swap_buf.at[0],
        swap_buf.at[1],
        gram_send.at[2],
        gram_recv.at[2],
        device_id=partner,
        device_id_type=MESH,
    )
    swap.start()
    swap.wait_recv()
    even = jnp.where(core == 0, swap_buf[0], swap_buf[1])
    odd = jnp.where(core == 0, swap_buf[1], swap_buf[0])
    dense = jnp.concatenate([even[0:4], odd[0:4]], axis=0)
    parts = [dense] + [pltpu.roll(dense, 128 - block * q, 1) for q in range(1, 4)]
    square = jnp.concatenate(parts, axis=0)
    square = jnp.where(
        lax.broadcasted_iota(jnp.int32, (block, 128), 1) < block, square, 0.0
    )
    gram = jnp.concatenate([square, jnp.zeros((8, 128), f32)], axis=0)
    extra = even[4:5]
    values = [extra] + [pltpu.roll(extra, 128 - keep * q, 1) for q in range(1, 3)]
    for q in range(3):
        gram = jnp.where(row_id == block + q, values[q], gram)
    for q in range(3):
        gram = jnp.where(lane_id == block + q, as_column(values[q]), gram)
    eye = jnp.where(row_id == lane_id, 2.0, 0.0)
    lower = jnp.logical_and(row_id < last, lane_id < last)
    matrix = jnp.where(lower, eye - gram, 0.0)

    scale_row = jnp.ones((1, 128), f32)
    scale_column = jnp.ones((ROWS, 1), f32)
    results = jnp.zeros((8, 128), f32)
    row_8 = lax.broadcasted_iota(jnp.int32, (8, 128), 0)
    lane_8 = lax.broadcasted_iota(jnp.int32, (8, 128), 1)
    inverse = None
    for step in range(STEPS):
        count = keep + step
        if step > 0:
            local_part(step)
            project(
                [(0, W[2]), (ROWS, V[last + step, 2])], 2, acc, 0, count, True
            )
            for plane in (3, 1, 0):
                project([(ROWS, V[last + step, plane])], plane, acc, 0, count, False)
            if step > 1:
                for plane in range(planes):
                    out[step - 2, plane] = V[last + step - 1, plane] * inverse
            finish_operator(step, count)
        sums = get_row(step)
        if step > 0:
            square = jnp.sum(
                jnp.where(lane_row == ROWS + count - 1, sums, 0.0),
                axis=1,
                keepdims=True,
            )
            norm = jnp.sqrt(square + EPSILON)
            inverse = 1.0 / norm
            scale_row = jnp.where(lane_row == count - 1, inverse, scale_row)
            scale_column = jnp.where(row_column == count - 1, inverse, scale_column)
            results = jnp.where(
                jnp.logical_and(row_8 == step - 1, lane_8 == count - 1), norm, results
            )
            factor = scale_row * inverse
        else:
            factor = scale_row
        valid = lane_row < count
        first = jnp.where(valid, sums * factor, 0.0)
        moved = jnp.where(valid, pltpu.roll(sums, 128 - ROWS, 1), 0.0)
        cross = moved * factor
        cross_column = as_column(moved) * scale_column
        if step > 0:
            cross_column = cross_column * inverse
        matrix = jnp.where(row_id == count - 1, eye - cross, matrix)
        matrix = jnp.where(lane_id == count - 1, eye - cross_column, matrix)
        weights = jnp.sum(matrix * first, axis=1, keepdims=True)
        weights = jnp.where(row_column < count, weights, 0.0)
        hb[...] = jnp.broadcast_to(weights * scale_column, hb.shape)

        def combine(plane, where):
            start = W[plane, where]
            if step > 0:
                start = start * inverse

            def minus(i, total):
                return total - hb[pl.ds(i, 1), :] * V[i, plane, where]

            def four(t, total):
                for q in range(4):
                    total = minus(4 * t + q, total)
                return total

            total = lax.fori_loop(0, count // 4, four, start)
            for i in range(4 * (count // 4), count):
                total = minus(i, total)
            V[count, plane, where] = total

        more = step + 1 < STEPS
        for plane in order:
            if more and plane >= planes - 2:
                for part in range(PIECES[plane]):
                    combine(plane, piece(plane, part))
                    send_piece(step + 1, plane, part)
            else:
                combine(plane, slice(None))
            if more:
                send_rest(step + 1, plane)
        results = jnp.where(row_8 == step, as_row(weights, ROWS), results)

    total = jnp.zeros((8, 128), f32)
    for plane in range(planes):
        v = V[keep + STEPS - 1, plane]
        total = total + folded(v * v)
    square = jnp.sum(jnp.sum(total, axis=0, keepdims=True), axis=1, keepdims=True)
    send_row(STEPS, jnp.broadcast_to(square, (1, 128)))
    for plane in range(planes):
        out[STEPS - 2, plane] = V[keep + STEPS - 2, plane] * inverse
    sums = get_row(STEPS)
    norm = jnp.sqrt(sums[:, 0:1] + EPSILON)
    inverse = 1.0 / norm
    results = jnp.where(
        jnp.logical_and(row_8 == STEPS - 1, lane_8 == keep + STEPS - 1), norm, results
    )
    hess[...] = results[0:STEPS, 0:ROWS]
    for plane in range(planes):
        out[STEPS - 1, plane] = V[keep + STEPS - 1, plane] * inverse

    for step in range(STEPS):

        @pl.when(chip < CHIPS - 1)
        def _():
            for plane in (planes - 2, planes - 1):
                for part in range(PIECES[plane]):
                    to_next(step, plane, part).wait_send()

        @pl.when(chip > 0)
        def _():
            to_previous(step).wait_send()

        for plane in range(planes):
            to_side(step, plane).wait_send()
    for n in range(STEPS + 1):
        row_bytes(n, row_send).wait()
    to_pair.wait_send()
    half_bytes(gram_send).wait()
    swap.wait_send()


def put_out(vectors, columns, vectors_out, columns_out, sem):
    copies = [
        pltpu.make_async_copy(vectors, vectors_out, sem.at[0]),
        pltpu.make_async_copy(columns, columns_out, sem.at[1]),
    ]
    for copy in copies:
        copy.start()
    for copy in copies:
        copy.wait()


def body(basis_vectors, reaction):
    keep, planes, rows, cols = basis_vectors.shape
    f32 = jnp.float32
    field = (planes, rows, cols)
    dma = pltpu.SemaphoreType.DMA
    vmem = pltpu.VMEM
    reaction = pltpu.with_memory_space_constraint(reaction, pltpu.HBM)
    vectors, columns = pl.pallas_call(
        functools.partial(kernel, keep, planes, rows, cols),
        out_shape=(
            jax.ShapeDtypeStruct((STEPS, *field), f32),
            jax.ShapeDtypeStruct((STEPS, keep + STEPS), f32),
        ),
        in_specs=[pl.BlockSpec(memory_space=pltpu.HBM)] * 2,
        out_specs=(
            pl.BlockSpec(memory_space=pltpu.VMEM),
            pl.BlockSpec(memory_space=pltpu.VMEM),
        ),
        scratch_shapes=[
            vmem((keep + STEPS, *field), f32),
            vmem(field, f32),
            vmem(field, f32),
            vmem((STEPS, 2, rows, cols), f32),
            vmem((STEPS, rows, cols), f32),
            vmem((STEPS, planes, 8, cols), f32),
            vmem((2 * ROWS, 8, 128), f32),
            vmem((3 * ROWS, 8, 128), f32),
            vmem((8 * keep, 256), f32),
            vmem((8 * keep, 256), f32),
            vmem((8 * keep - 256, 256), f32),
            vmem((256, 128), f32),
            vmem((ROWS, cols), f32),
            vmem((STEPS + 1, 1, 128), f32),
            vmem((STEPS + 1, DEVICES, 1, 128), f32),
            vmem((16, 128), f32),
            vmem((8, 128), f32),
            vmem((8, 128), f32),
            vmem((CHIPS, 8, 128), f32),
            vmem((2, 5, 128), f32),
            dma((9,)),
            dma((STEPS, 2, 4)),
            dma((STEPS,)),
            dma((STEPS, 2, 4)),
            dma((STEPS,)),
            dma((STEPS, planes)),
            dma((STEPS, planes)),
            dma((STEPS + 1,)),
            dma((STEPS + 1,)),
            dma((3,)),
            dma((3,)),
        ],
        compiler_params=pltpu.CompilerParams(
            collective_id=0,
            has_side_effects=True,
            vmem_limit_bytes=48 * 1024 * 1024,
        ),
    )(basis_vectors, reaction)
    shapes = (vectors, columns)
    new_vectors, rows_out = pl.pallas_call(
        put_out,
        out_shape=tuple(jax.ShapeDtypeStruct(a.shape, f32) for a in shapes),
        in_specs=[pl.BlockSpec(memory_space=pltpu.VMEM)] * 2,
        out_specs=(pl.BlockSpec(memory_space=pl.ANY),) * 2,
        scratch_shapes=[dma((2,))],
        compiler_params=pltpu.CompilerParams(vmem_limit_bytes=4 * 1024 * 1024),
    )(vectors, columns)
    return new_vectors, rows_out.T


def solution(mesh):
    return jax.shard_map(
        body,
        mesh=mesh,
        in_specs=(P(None, "gx", "gy", None), P("gx", "gy", None)),
        out_specs=(P(None, "gx", "gy", None), P()),
        check_vma=False,
    )
```
